256 devices in a mesh: frames: 8 (over x, core), codes: 32 (over y, z).
Axes of the slice: x: 4, y: 4, z: 8, core: 2. Of those that a mesh axis runs over, the one named last changes fastest.
Arguments:
- hidden: bfloat16 [32768, 1024], P('frames'), may hold values from -5 to 5
- head: bfloat16 [1024, 8192], P('frames', 'codes'), may hold values from -2 to 2
- chosen: int32 [8, 32768], P(None, 'frames'), may hold values from 0 to 1023
Outputs:
- confidence: float32 [8, 32768], P(None, 'frames')
- entropy: float32 [8, 32768], P(None, 'frames')
The draws below stay inside these ranges and needn't reach their ends.
All inputs are finite; a program needn't handle non-finite values.
Results may differ from the reference program's by a relative error of at most 0.0003.
Values may be sent and summed in bfloat16 or wider, within the bound.
A program may use at most 64 MiB of HBM per device.

```python
import math
import jax
import jax.numpy as jnp

D = 1024
CODES = 1024
LEVELS = 8
FRAMES = 32768


def draw_hidden(key, part):
    seeded = jax.random.fold_in(key, 11)
    subkeys = jax.random.split(seeded, 2)
    values = jnp.clip(jax.random.normal(subkeys[1], (FRAMES, D), jnp.float32), -5.0, 5.0)
    return values.astype(jnp.bfloat16)


def draw_head(key, part):
    seeded = jax.random.fold_in(key, 13)
    subkeys = jax.random.split(seeded, 2)
    spread = 3.0 / math.sqrt(D)
    values = jnp.clip(jax.random.normal(subkeys[1], (D, LEVELS * CODES), jnp.float32) * spread, -6.0 * spread, 6.0 * spread)
    return values.astype(jnp.bfloat16)


def set_ends(values, own_key, low, largest):
    dims = values.shape
    index_at = [jax.random.randint(jax.random.fold_in(own_key, axis), (), 0, dims[axis]) for axis in range(len(dims))]
    values = values.at[tuple(index_at)].set(low)
    longest = dims.index(max(dims))
    index_at[longest] = (index_at[longest] + 1) % dims[longest]
    return values.at[tuple(index_at)].set(largest)


def setup_inputs(seed: int = 0) -> dict:
    arg_keys = jax.random.split(jax.random.key(seed), 4)
    return {
        "hidden": draw_hidden(jax.random.fold_in(arg_keys[3], 71), 0),
        "head": draw_head(jax.random.fold_in(arg_keys[3], 71), 0),
        "chosen": set_ends(jax.random.randint(arg_keys[2], (LEVELS, FRAMES), 0, CODES), jax.random.fold_in(arg_keys[2], 1), 0, CODES - 1).astype(jnp.int32),
    }


def reference(hidden, head, chosen):
    confidences = []
    entropies = []
    for level_id in range(LEVELS):
        head_slice = head[:, level_id * CODES:(level_id + 1) * CODES]
        scores = jnp.dot(hidden, head_slice, preferred_element_type=jnp.float32)
        highest = jnp.max(scores, axis=1)
        shifted = jnp.exp(scores - highest[:, None])
        exp_total = jnp.sum(shifted, axis=1)
        exp_logit = jnp.sum(shifted * scores, axis=1)
        log_total = highest + jnp.log(exp_total)
        wanted = chosen[level_id][:, None].astype(jnp.int32)
        picked = jnp.take_along_axis(scores, wanted, axis=1)[:, 0]
        confidences.append(picked - log_total)
        entropies.append(log_total - exp_logit / exp_total)
    return jnp.stack(confidences), jnp.stack(entropies)
```

```python
import functools
import math

import jax
import jax.numpy as jnp
from jax import lax
from jax.experimental import pallas as pl
from jax.experimental.pallas import tpu as pltpu
from jax.sharding import PartitionSpec as P

CODES = 1024
LOG2E = math.log2(math.e)
LN2 = math.log(2.0)
MESH = pl.DeviceIdType.MESH
LANES = 128
TILE = 256


def tile_stats(scaled, wanted):
    flipped = scaled.T
    columns, frames = flipped.shape
    top = jnp.max(flipped, axis=0, keepdims=True)
    below = flipped - top
    powers = jnp.exp2(below)
    total = jnp.sum(powers, axis=0, keepdims=True)
    weighted = jnp.sum(powers * below, axis=0, keepdims=True)
    groups = columns // 8
    pool = flipped.reshape(groups, 8, frames)
    spread = jnp.broadcast_to(wanted, (8, frames))
    bit = groups.bit_length() - 2
    while bit >= 0:
        half = 1 << bit
        upper = (lax.shift_right_arithmetic(spread, 3 + bit) & 1) == 1
        pool = jnp.where(upper[None], pool[half:], pool[:half])
        bit -= 1
    row = lax.broadcasted_iota(jnp.int32, (8, frames), 0)
    here = (row == (spread & 7)) & (spread >= 0) & (spread < columns)
    picked = jnp.sum(jnp.where(here, pool[0], 0.0), axis=0, keepdims=True)
    return top, total, weighted, picked


def kernel(
    xs, ys, zs,
    hidden_hbm, head_hbm, chosen_ref, conf_ref, ent_ref,
    hid, weights, acc, outgoing, incoming, final,
    load_sem, wsend, wrecv, ssend, srecv, gsend, gzrecv, gyrecv,
):
    fidx = lax.axis_index("frames")
    cidx = lax.axis_index("codes")
    x, core = fidx // 2, fidx % 2
    y, z = cidx // zs, cidx % zs
    q, quad = z % 4, z // 4
    level = y * (zs // 4) + quad
    sib = 1 - core
    xl, xr, xo = (x + xs - 1) % xs, (x + 1) % xs, (x + 2) % xs

    def at(px, pcore, py, pz):
        return (px * 2 + pcore, py * zs + pz)

    own_head = pltpu.make_async_copy(head_hbm, weights.at[fidx], load_sem.at[0])
    own_head.start()
    quarter = hid.shape[0] // 4
    loads = []
    for i in range(4):
        rows = pl.ds(i * quarter, quarter)
        copy = pltpu.make_async_copy(hidden_hbm.at[rows], hid.at[rows], load_sem.at[1 + i])
        copy.start()
        loads.append(copy)

    z_peers = [(z + d) % zs for d in (1, zs - 1, 2, zs - 2, 3, zs - 3, 4)]
    y_peers = [(y + d) % ys for d in (1, ys - 1, 2)]
    barrier = pltpu.get_barrier_semaphore()
    peers = [at(x, sib, y, z), at(xl, core, y, z), at(xr, core, y, z)]
    peers += [at(x, core, y, pz) for pz in z_peers]
    peers += [at(x, core, py, z) for py in y_peers]
    for peer in peers:
        pl.semaphore_signal(barrier, inc=1, device_id=peer, device_id_type=MESH)
    pl.semaphore_wait(barrier, len(peers))
    own_head.wait()

    half = weights.shape[1] // 2

    def piece(slot, part):
        if part is None:
            return weights.at[slot]
        return weights.at[slot, pl.ds(part * half, half)]

    sends = []

    def push(slot, part, index, peer):
        copy = pltpu.make_async_remote_copy(
            src_ref=piece(slot, part), dst_ref=piece(slot, part),
            send_sem=wsend.at[index], recv_sem=wrecv.at[index],
            device_id=peer, device_id_type=MESH,
        )
        copy.start()
        sends.append(copy)

    def landed(slot, part, index):
        pltpu.make_async_remote_copy(
            src_ref=piece(slot, part), dst_ref=piece(slot, part),
            send_sem=wsend.at[index], recv_sem=wrecv.at[index],
            device_id=at(x, sib, y, z), device_id_type=MESH,
        ).wait_recv()

    mate = at(x, sib, y, z)
    left, right = at(xl, core, y, z), at(xr, core, y, z)
    push(fidx, 0, 1, right)
    push(fidx, 1, 4, left)
    push(fidx, None, 0, mate)
    push(fidx, 1, 2, right)
    push(fidx, 0, 3, left)
    left_slot, right_slot, far_slot = xl * 2 + core, xr * 2 + core, xo * 2 + core
    landed(left_slot, 0, 1)
    push(left_slot, 0, 5, right)
    landed(right_slot, 1, 4)
    push(right_slot, 1, 6, left)
    landed(left_slot, 1, 2)
    push(left_slot, None, 7, mate)
    landed(right_slot, 0, 3)
    push(right_slot, None, 8, mate)

    depth = 2 * weights.shape[1]

    def product(rows, chip):
        pair = weights[pl.ds(chip * 2, 2)].reshape(depth, weights.shape[2])
        cols = pl.ds(pl.multiple_of(chip * depth, depth), depth)
        return jnp.dot(hid[rows, cols], pair, preferred_element_type=jnp.float32)

    landed(x * 2 + sib, None, 0)
    step = 512
    for i in range(4):
        loads[i].wait()
    for i in range(hid.shape[0] // step):
        rows = pl.ds(i * step, step)
        acc[rows] = product(rows, x)
    landed(far_slot, 0, 5)
    push(far_slot, 0, 9, mate)
    landed(far_slot, 1, 6)
    push(far_slot, 1, 10, mate)
    landed(xl * 2 + sib, None, 7)
    landed(xr * 2 + sib, None, 8)
    for i in range(hid.shape[0] // step):
        rows = pl.ds(i * step, step)
        acc[rows] += product(rows, xl) + product(rows, xr)
    landed(xo * 2 + sib, 0, 9)
    landed(xo * 2 + sib, 1, 10)

    offset = q * weights.shape[2]
    low = q < 2
    order = [jnp.where(low, 3, 0), jnp.where(low, 2, 1)]
    order.append(jnp.where(low, jnp.where(q == 1, 0, 1), jnp.where(q == 2, 3, 2)))
    order.append(q)
    stat_sends = []
    for s in range(4):
        part = order[s]
        for t in range(quarter // TILE):
            rows = pl.ds(pl.multiple_of(part * quarter + t * TILE, TILE), TILE)
            scaled = (acc[rows] + product(rows, xo)) * LOG2E
            wanted = chosen_ref[pl.ds(level, 1), rows] - offset
            stats = tile_stats(scaled, wanted)
            for k in range(4):
                for i in range(TILE // LANES):
                    outgoing[part, k, pl.ds(t * (TILE // LANES) + i, 1), :] = stats[k][:, i * LANES:(i + 1) * LANES]
        if s < 3:
            copy = pltpu.make_async_remote_copy(
                src_ref=outgoing.at[part], dst_ref=incoming.at[q],
                send_sem=ssend.at[s], recv_sem=srecv.at[q],
                device_id=at(x, core, y, quad * 4 + part), device_id_type=MESH,
            )
            copy.start()
            stat_sends.append(copy)

    found = [tuple(outgoing[q, k] for k in range(4))]
    for s in range(3):
        part = order[s]
        pltpu.make_async_remote_copy(
            src_ref=outgoing.at[part], dst_ref=incoming.at[part],
            send_sem=ssend.at[s], recv_sem=srecv.at[part],
            device_id=at(x, core, y, quad * 4 + part), device_id_type=MESH,
        ).wait_recv()
        found.append(tuple(incoming[part, k] for k in range(4)))
    top = functools.reduce(jnp.maximum, [f[0] for f in found])
    total = weighted = picked = jnp.zeros_like(top)
    for own_top, own_total, own_weighted, own_picked in found:
        gap = own_top - top
        factor = jnp.exp2(gap)
        total += factor * own_total
        weighted += factor * (own_weighted + gap * own_total)
        picked += own_picked
    bits = jnp.log(total)
    final[cidx, 0] = (picked - top) * LN2 - bits
    final[cidx, 1] = bits - LN2 * (weighted / total)

    z_offsets = (1, zs - 1, 2, zs - 2, 3, zs - 3, 4)
    last = []

    def spread(block, index, recv, peer):
        copy = pltpu.make_async_remote_copy(
            src_ref=final.at[block], dst_ref=final.at[block],
            send_sem=gsend.at[index], recv_sem=recv,
            device_id=peer, device_id_type=MESH,
        )
        copy.start()
        last.append(copy)

    def arrived(block, recv):
        pltpu.make_async_remote_copy(
            src_ref=final.at[block], dst_ref=final.at[block],
            send_sem=gsend.at[0], recv_sem=recv,
            device_id=mate, device_id_type=MESH,
        ).wait_recv()

    for n, d in enumerate(reversed(z_offsets)):
        spread(cidx, n, gzrecv.at[d], at(x, core, y, (z + d) % zs))
    y_offsets = (2, 1, ys - 1)
    count = len(z_offsets)

    def onward(pz, d_index):
        nonlocal count
        for d in y_offsets:
            spread(y * zs + pz, count, gyrecv.at[d, d_index], at(x, core, (y + d) % ys, z))
            count += 1

    onward(z, 0)
    for d in z_offsets:
        pz = (z + zs - d) % zs
        arrived(y * zs + pz, gzrecv.at[d])
        onward(pz, d)
    for d in (1, ys - 1, 2):
        py = (y + ys - d) % ys
        for dz in (0,) + z_offsets:
            arrived(py * zs + (z + zs - dz) % zs, gyrecv.at[d, dz])

    blocks = final.shape[0]
    levels = conf_ref.shape[0]
    for part in range(4):
        for j in range(8):
            cols = pl.ds(part * quarter + j * LANES, LANES)
            for k, out in ((0, conf_ref), (1, ent_ref)):
                out[:, cols] = jnp.concatenate(
                    [final[g * 4 + part, k, pl.ds(j, 1), :] for g in range(levels)], axis=0
                )
    for copy in sends + stat_sends + last:
        copy.wait_send()


def on_device(xs, ys, zs, hidden, head, chosen):
    rows, width = hidden.shape
    depth, columns = head.shape
    levels = chosen.shape[0]
    quarter = rows // 4
    dma = pltpu.SemaphoreType.DMA
    out = jax.ShapeDtypeStruct((levels, rows), jnp.float32)
    vmem = pl.BlockSpec(memory_space=pltpu.VMEM)
    anywhere = pl.BlockSpec(memory_space=pl.ANY)
    return pl.pallas_call(
        functools.partial(kernel, xs, ys, zs),
        out_shape=(out, out),
        in_specs=[anywhere, anywhere, vmem],
        out_specs=(vmem, vmem),
        scratch_shapes=[
            pltpu.VMEM((rows, width), jnp.bfloat16),
            pltpu.VMEM((width // depth, depth, columns), jnp.bfloat16),
            pltpu.VMEM((rows, columns), jnp.float32),
            pltpu.VMEM((4, 4, quarter // LANES, LANES), jnp.float32),
            pltpu.VMEM((4, 4, quarter // LANES, LANES), jnp.float32),
            pltpu.VMEM((ys * zs, 2, quarter // LANES, LANES), jnp.float32),
            dma((5,)), dma((11,)), dma((11,)), dma((3,)), dma((4,)), dma((31,)), dma((8,)), dma((4, 8)),
        ],
        compiler_params=pltpu.CompilerParams(collective_id=0, has_side_effects=True),
    )(hidden, head, chosen)


def solution(mesh):
    return jax.shard_map(
        functools.partial(on_device, mesh.shape["frames"] // 2, 4, mesh.shape["codes"] // 4),
        mesh=mesh,
        in_specs=(P("frames", None), P("frames", "codes"), P(None, "frames")),
        out_specs=(P(None, "frames"), P(None, "frames")),
        check_vma=False,
    )
```

```python
import functools
import math

import jax
import jax.numpy as jnp
from jax import lax
from jax.experimental import pallas as pl
from jax.experimental.pallas import tpu as pltpu
from jax.sharding import PartitionSpec as P

CODES = 1024
LOG2E = math.log2(math.e)
LN2 = math.log(2.0)
MESH = pl.DeviceIdType.MESH
LANES = 128
TILE = 256
PROFILE = False


open_scopes = []


def mark(name):
    if PROFILE:
        while open_scopes:
            open_scopes.pop().__exit__(None, None, None)
        if name:
            open_scopes.append(jax.named_scope(name))
            open_scopes[-1].__enter__()


def tile_stats(scaled, wanted):
    flipped = scaled.T
    columns, frames = flipped.shape
    top = jnp.max(flipped, axis=0, keepdims=True)
    below = flipped - top
    powers = jnp.exp2(below)
    total = jnp.sum(powers, axis=0, keepdims=True)
    weighted = jnp.sum(powers * below, axis=0, keepdims=True)
    groups = columns // 8
    pool = flipped.reshape(groups, 8, frames)
    spread = jnp.broadcast_to(wanted, (8, frames))
    bit = groups.bit_length() - 2
    while bit >= 0:
        half = 1 << bit
        upper = (lax.shift_right_arithmetic(spread, 3 + bit) & 1) == 1
        pool = jnp.where(upper[None], pool[half:], pool[:half])
        bit -= 1
    row = lax.broadcasted_iota(jnp.int32, (8, frames), 0)
    here = (row == (spread & 7)) & (spread >= 0) & (spread < columns)
    picked = jnp.sum(jnp.where(here, pool[0], 0.0), axis=0, keepdims=True)
    return top, total, weighted, picked


def kernel(
    xs, ys, zs,
    hidden_hbm, head_hbm, chosen_hbm, final,
    hid, weights, acc, outgoing, incoming, chosen_ref,
    load_sem, wsend, wrecv, ssend, srecv, gsend, gzrecv, gyrecv, near_sem, wide_sem, side_sem,
):
    fidx = lax.axis_index("frames")
    cidx = lax.axis_index("codes")
    x, core = fidx // 2, fidx % 2
    y, z = cidx // zs, cidx % zs
    q, quad = z % 4, z // 4
    level = y * (zs // 4) + quad
    sib = 1 - core
    xl, xr, xo = (x + xs - 1) % xs, (x + 1) % xs, (x + 2) % xs

    def at(px, pcore, py, pz):
        return (px * 2 + pcore, py * zs + pz)

    mark("p00issue")
    own_head = pltpu.make_async_copy(head_hbm, weights.at[fidx], load_sem.at[0])
    own_head.start()
    chosen_load = pltpu.make_async_copy(chosen_hbm, chosen_ref, load_sem.at[5])
    quarter = hid.shape[0] // 4
    loads = []
    for i in range(4):
        rows = pl.ds(i * quarter, quarter)
        copy = pltpu.make_async_copy(hidden_hbm.at[rows], hid.at[rows], load_sem.at[1 + i])
        copy.start()
        loads.append(copy)

    mark("p01barrier")
    mate = at(x, sib, y, z)
    left, right = at(xl, core, y, z), at(xr, core, y, z)
    z_near = [at(x, core, y, (z + d) % zs) for d in (1, zs - 1)]
    z_wide = [at(x, core, y, (z + d) % zs) for d in (2, zs - 2)]
    y_near = [at(x, core, (y + d) % ys, z) for d in (1, ys - 1)]
    barrier = pltpu.get_barrier_semaphore()
    around = [mate, left, right, at(xo, core, y, z)] + z_near + y_near
    for peer in around:
        pl.semaphore_signal(barrier, inc=1, device_id=peer, device_id_type=MESH)
    chosen_load.start()
    pl.semaphore_wait(barrier, len(around))
    for peer in z_near:
        pl.semaphore_signal(near_sem, inc=1, device_id=peer, device_id_type=MESH)
    for peer in y_near:
        pl.semaphore_signal(side_sem, inc=1, device_id=peer, device_id_type=MESH)
    own_head.wait()

    mark("p02gather")
    half = weights.shape[1] // 2

    def piece(slot, part):
        if part is None:
            return weights.at[slot]
        return weights.at[slot, pl.ds(part * half, half)]

    sends = []

    def push(slot, part, index, peer):
        copy = pltpu.make_async_remote_copy(
            src_ref=piece(slot, part), dst_ref=piece(slot, part),
            send_sem=wsend.at[index], recv_sem=wrecv.at[index],
            device_id=peer, device_id_type=MESH,
        )
        copy.start()
        sends.append(copy)

    def landed(slot, part, index):
        pltpu.make_async_remote_copy(
            src_ref=piece(slot, part), dst_ref=piece(slot, part),
            send_sem=wsend.at[index], recv_sem=wrecv.at[index],
            device_id=at(x, sib, y, z), device_id_type=MESH,
        ).wait_recv()

    push(fidx, None, 0, mate)
    push(fidx, None, 1, right)
    push(fidx, None, 2, left)
    push(fidx, None, 3, at(xo, core, y, z))
    pl.semaphore_wait(near_sem, 2)
    for peer in z_wide:
        pl.semaphore_signal(wide_sem, inc=1, device_id=peer, device_id_type=MESH)
    left_slot, right_slot, far_slot = xl * 2 + core, xr * 2 + core, xo * 2 + core
    landed(left_slot, None, 1)
    push(left_slot, None, 4, mate)
    landed(right_slot, None, 2)
    push(right_slot, None, 5, mate)

    mark("p03ownmm")
    depth = 2 * weights.shape[1]

    def product(rows, chip):
        pair = weights[pl.ds(chip * 2, 2)].reshape(depth, weights.shape[2])
        cols = pl.ds(pl.multiple_of(chip * depth, depth), depth)
        return jnp.dot(hid[rows, cols], pair, preferred_element_type=jnp.float32)

    landed(x * 2 + sib, None, 0)
    step = 512
    for i in range(4):
        loads[i].wait()
    for i in range(hid.shape[0] // step):
        rows = pl.ds(i * step, step)
        acc[rows] = product(rows, x)
    mark("p04far")
    landed(far_slot, None, 3)
    push(far_slot, None, 6, mate)
    mark("p05sidemm")
    landed(xl * 2 + sib, None, 4)
    landed(xr * 2 + sib, None, 5)
    for i in range(hid.shape[0] // step):
        rows = pl.ds(i * step, step)
        acc[rows] += product(rows, xl) + product(rows, xr)
    mark("p06farwait")
    landed(xo * 2 + sib, None, 6)

    mark("p07stats")
    pl.semaphore_wait(wide_sem, 2)
    pl.semaphore_wait(side_sem, 2)
    chosen_load.wait()
    offset = q * weights.shape[2]
    low = q < 2
    order = [jnp.where(low, 3, 0), jnp.where(low, 2, 1)]
    order.append(jnp.where(low, jnp.where(q == 1, 0, 1), jnp.where(q == 2, 3, 2)))
    order.append(q)
    stat_sends = []
    for s in range(4):
        part = order[s]
        for t in range(quarter // TILE):
            rows = pl.ds(pl.multiple_of(part * quarter + t * TILE, TILE), TILE)
            scaled = (acc[rows] + product(rows, xo)) * LOG2E
            wanted = chosen_ref[pl.ds(level, 1), rows] - offset
            stats = tile_stats(scaled, wanted)
            for k in range(4):
                for i in range(TILE // LANES):
                    outgoing[part, k, pl.ds(t * (TILE // LANES) + i, 1), :] = stats[k][:, i * LANES:(i + 1) * LANES]
        if s < 3:
            copy = pltpu.make_async_remote_copy(
                src_ref=outgoing.at[part], dst_ref=incoming.at[q],
                send_sem=ssend.at[s], recv_sem=srecv.at[q],
                device_id=at(x, core, y, quad * 4 + part), device_id_type=MESH,
            )
            copy.start()
            stat_sends.append(copy)

    mark("p08statwait")
    found = [tuple(outgoing[q, k] for k in range(4))]
    for s in range(3):
        part = order[s]
        pltpu.make_async_remote_copy(
            src_ref=outgoing.at[part], dst_ref=incoming.at[part],
            send_sem=ssend.at[s], recv_sem=srecv.at[part],
            device_id=at(x, core, y, quad * 4 + part), device_id_type=MESH,
        ).wait_recv()
        found.append(tuple(incoming[part, k] for k in range(4)))
    top = functools.reduce(jnp.maximum, [f[0] for f in found])
    total = weighted = picked = jnp.zeros_like(top)
    for own_top, own_total, own_weighted, own_picked in found:
        gap = own_top - top
        factor = jnp.exp2(gap)
        total += factor * own_total
        weighted += factor * (own_weighted + gap * own_total)
        picked += own_picked
    bits = jnp.log(total)
    final[cidx, 0] = (picked - top) * LN2 - bits
    final[cidx, 1] = bits - LN2 * (weighted / total)

    mark("p09spread")
    z_offsets = (1, zs - 1, 2, zs - 2, 3, zs - 3, 4)
    last = []

    def spread(block, index, recv, peer):
        copy = pltpu.make_async_remote_copy(
            src_ref=final.at[block], dst_ref=final.at[block],
            send_sem=gsend.at[index], recv_sem=recv,
            device_id=peer, device_id_type=MESH,
        )
        copy.start()
        last.append(copy)

    def arrived(block, recv):
        pltpu.make_async_remote_copy(
            src_ref=final.at[block], dst_ref=final.at[block],
            send_sem=gsend.at[0], recv_sem=recv,
            device_id=mate, device_id_type=MESH,
        ).wait_recv()

    for n, d in enumerate(reversed(z_offsets)):
        spread(cidx, n, gzrecv.at[d], at(x, core, y, (z + d) % zs))
    y_offsets = (2, 1, ys - 1)
    count = len(z_offsets)

    def onward(pz, d_index):
        nonlocal count
        for d in y_offsets:
            spread(y * zs + pz, count, gyrecv.at[d, d_index], at(x, core, (y + d) % ys, z))
            count += 1

    onward(z, 0)
    for d in z_offsets:
        pz = (z + zs - d) % zs
        arrived(y * zs + pz, gzrecv.at[d])
        onward(pz, d)
    mark("p10ywait")
    for d in (1, ys - 1, 2):
        py = (y + ys - d) % ys
        for dz in (0,) + z_offsets:
            arrived(py * zs + (z + zs - dz) % zs, gyrecv.at[d, dz])

    mark("p11drain")
    for copy in sends + stat_sends + last:
        copy.wait_send()
    mark(None)


def lay_out(final, conf_hbm, ent_hbm, conf, ent, sems):
    levels, rows = conf.shape
    copies = []
    for k, (out, dst) in enumerate(((conf, conf_hbm), (ent, ent_hbm))):
        for part in range(4):
            for j in range(rows // 4 // LANES):
                cols = pl.ds(part * (rows // 4) + j * LANES, LANES)
                out[:, cols] = jnp.concatenate(
                    [final[g * 4 + part, k, pl.ds(j, 1), :] for g in range(levels)], axis=0
                )
        copy = pltpu.make_async_copy(out, dst, sems.at[k])
        copy.start()
        copies.append(copy)
    for copy in copies:
        copy.wait()


def on_device(xs, ys, zs, hidden, head, chosen):
    rows, width = hidden.shape
    depth, columns = head.shape
    levels = chosen.shape[0]
    quarter = rows // 4
    dma = pltpu.SemaphoreType.DMA
    out = jax.ShapeDtypeStruct((levels, rows), jnp.float32)
    vmem = pl.BlockSpec(memory_space=pltpu.VMEM)
    anywhere = pl.BlockSpec(memory_space=pltpu.HBM)
    final = pl.pallas_call(
        functools.partial(kernel, xs, ys, zs),
        out_shape=pltpu.VMEM((ys * zs, 2, quarter // LANES, LANES), jnp.float32),
        in_specs=[anywhere, anywhere, anywhere],
        out_specs=vmem,
        scratch_shapes=[
            pltpu.VMEM((rows, width), jnp.bfloat16),
            pltpu.VMEM((width // depth, depth, columns), jnp.bfloat16),
            pltpu.VMEM((rows, columns), jnp.float32),
            pltpu.VMEM((4, 4, quarter // LANES, LANES), jnp.float32),
            pltpu.VMEM((4, 4, quarter // LANES, LANES), jnp.float32),
            pltpu.VMEM((levels, rows), jnp.int32),
            dma((6,)), dma((11,)), dma((11,)), dma((3,)), dma((4,)), dma((31,)), dma((8,)), dma((4, 8)),
            pltpu.SemaphoreType.REGULAR, pltpu.SemaphoreType.REGULAR, pltpu.SemaphoreType.REGULAR,
        ],
        compiler_params=pltpu.CompilerParams(collective_id=0, has_side_effects=True, vmem_limit_bytes=56 << 20),
    )(hidden, head, chosen)
    return pl.pallas_call(
        lay_out,
        out_shape=(out, out),
        in_specs=[vmem],
        out_specs=(anywhere, anywhere),
        scratch_shapes=[pltpu.VMEM((levels, rows), jnp.float32)] * 2 + [dma((2,))],
        compiler_params=pltpu.CompilerParams(vmem_limit_bytes=4 << 20),
    )(final)


def solution(mesh):
    return jax.shard_map(
        functools.partial(on_device, mesh.shape["frames"] // 2, 4, mesh.shape["codes"] // 4),
        mesh=mesh,
        in_specs=(P("frames", None), P("frames", "codes"), P(None, "frames")),
        out_specs=(P(None, "frames"), P(None, "frames")),
        check_vma=False,
    )
```

```python
import functools
import math

import jax
import jax.numpy as jnp
from jax import lax
from jax.experimental import pallas as pl
from jax.experimental.pallas import tpu as pltpu
from jax.sharding import PartitionSpec as P

CODES = 1024
LOG2E = math.log2(math.e)
LN2 = math.log(2.0)
MESH = pl.DeviceIdType.MESH
LANES = 128
TILE = 128
BLOCK = 256
PUSHES = 7
CONF_CODE = (64.0, 20500.0)
ENT_CODE = (1024.0, 6.95)
PROFILE = False


open_scopes = []


def mark(name):
    if PROFILE:
        while open_scopes:
            open_scopes.pop().__exit__(None, None, None)
        if name:
            open_scopes.append(jax.named_scope(name))
            open_scopes[-1].__enter__()


def tile_stats(scaled, wanted):
    flipped = scaled.T
    columns, frames = flipped.shape
    top = jnp.max(flipped, axis=0, keepdims=True)
    below = flipped - top
    powers = jnp.exp2(below)
    total = jnp.sum(powers, axis=0, keepdims=True)
    weighted = jnp.sum(powers * below, axis=0, keepdims=True)
    groups = columns // 8
    pool = flipped.reshape(groups, 8, frames)
    spread = jnp.broadcast_to(wanted, (8, frames))
    bit = groups.bit_length() - 2
    while bit >= 0:
        half = 1 << bit
        upper = (lax.shift_right_arithmetic(spread, 3 + bit) & 1) == 1
        pool = jnp.where(upper[None], pool[half:], pool[:half])
        bit -= 1
    row = lax.broadcasted_iota(jnp.int32, (8, frames), 0)
    here = (row == (spread & 7)) & (spread >= 0) & (spread < columns)
    picked = jnp.sum(jnp.where(here, pool[0], 0.0), axis=0, keepdims=True)
    return top, total, weighted, picked


def kernel(
    xs, ys, zs,
    hidden_hbm, head_hbm, chosen_hbm, words,
    hid, weights, acc, stage_a, stage_b, outgoing, incoming, chosen_ref,
    load_sem, wsend, wrecv, ssend, srecv, gsend, grecv, near_sem, wide_sem, side_sem, line_sem,
):
    fidx = lax.axis_index("frames")
    cidx = lax.axis_index("codes")
    x, core = fidx // 2, fidx % 2
    y, z = cidx // zs, cidx % zs
    q, quad = z % 4, z // 4
    level = y * (zs // 4) + quad
    sib = 1 - core
    xl, xr, xo = (x + xs - 1) % xs, (x + 1) % xs, (x + 2) % xs

    def at(px, pcore, py, pz):
        return (px * 2 + pcore, py * zs + pz)

    mark("p00issue")
    own_head = pltpu.make_async_copy(head_hbm, weights.at[fidx], load_sem.at[0])
    own_head.start()
    chosen_load = pltpu.make_async_copy(chosen_hbm, chosen_ref, load_sem.at[5])
    quarter = hid.shape[0] // 4
    loads = []
    for i in range(4):
        rows = pl.ds(i * quarter, quarter)
        copy = pltpu.make_async_copy(hidden_hbm.at[rows], hid.at[rows], load_sem.at[1 + i])
        copy.start()
        loads.append(copy)

    mark("p01barrier")
    mate = at(x, sib, y, z)
    left, right = at(xl, core, y, z), at(xr, core, y, z)
    z_near = [at(x, core, y, (z + d) % zs) for d in (1, zs - 1)]
    z_wide = [at(x, core, y, (z + d) % zs) for d in (2, zs - 2)]
    y_near = [at(x, core, (y + d) % ys, z) for d in (1, ys - 1)]
    barrier = pltpu.get_barrier_semaphore()
    around = [mate, left, right, at(xo, core, y, z)] + z_near + y_near
    for peer in around:
        pl.semaphore_signal(barrier, inc=1, device_id=peer, device_id_type=MESH)
    chosen_load.start()
    pl.semaphore_wait(barrier, len(around))
    for peer in z_near:
        pl.semaphore_signal(near_sem, inc=1, device_id=peer, device_id_type=MESH)
    for peer in y_near:
        pl.semaphore_signal(side_sem, inc=1, device_id=peer, device_id_type=MESH)
    own_head.wait()

    mark("p02gather")
    half = weights.shape[1] // 2

    def piece(slot, part):
        if part is None:
            return weights.at[slot]
        return weights.at[slot, pl.ds(part * half, half)]

    def push(slot, part, index, peer):
        copy = pltpu.make_async_remote_copy(
            src_ref=piece(slot, part), dst_ref=piece(slot, part),
            send_sem=wsend, recv_sem=wrecv.at[index],
            device_id=peer, device_id_type=MESH,
        )
        copy.start()

    def landed(slot, part, index):
        pltpu.make_async_remote_copy(
            src_ref=piece(slot, part), dst_ref=piece(slot, part),
            send_sem=wsend, recv_sem=wrecv.at[index],
            device_id=at(x, sib, y, z), device_id_type=MESH,
        ).wait_recv()

    push(fidx, None, 0, mate)
    push(fidx, None, 1, right)
    push(fidx, None, 2, left)
    push(fidx, None, 3, at(xo, core, y, z))
    pl.semaphore_wait(near_sem, 2)
    for peer in z_wide:
        pl.semaphore_signal(wide_sem, inc=1, device_id=peer, device_id_type=MESH)
    left_slot, right_slot, far_slot = xl * 2 + core, xr * 2 + core, xo * 2 + core
    depth = 2 * weights.shape[1]

    def product(rows, chip):
        pair = weights[pl.ds(chip * 2, 2)].reshape(depth, weights.shape[2])
        cols = pl.ds(pl.multiple_of(chip * depth, depth), depth)
        return jnp.dot(hid[rows, cols], pair, preferred_element_type=jnp.float32)

    mark("p03ownmm")
    landed(x * 2 + sib, None, 0)
    step = 512
    for i in range(4):
        loads[i].wait()
        for j in range(quarter // step):
            rows = pl.ds(i * quarter + j * step, step)
            acc[rows] = product(rows, x)
    mark("p04relay")
    landed(left_slot, None, 1)
    push(left_slot, None, 4, mate)
    landed(right_slot, None, 2)
    push(right_slot, None, 5, mate)
    landed(far_slot, None, 3)
    push(far_slot, None, 6, mate)
    mark("p05sidemm")
    landed(xl * 2 + sib, None, 4)
    for i in range(hid.shape[0] // step):
        rows = pl.ds(i * step, step)
        acc[rows] += product(rows, xl)
    mark("p06farwait")
    landed(xr * 2 + sib, None, 5)
    landed(xo * 2 + sib, None, 6)
    mark("p07stats")
    pl.semaphore_wait(wide_sem, 2)
    pl.semaphore_wait(side_sem, 2)
    for d in range(1, ys):
        pl.semaphore_signal(line_sem, inc=1, device_id=at(x, core, (y + d) % ys, z), device_id_type=MESH)
    chosen_load.wait()
    offset = q * weights.shape[2]
    low = q < 2
    order = [jnp.where(low, 3, 0), jnp.where(low, 2, 1)]
    order.append(jnp.where(low, jnp.where(q == 1, 0, 1), jnp.where(q == 2, 3, 2)))
    order.append(q)
    stages = (stage_a, stage_b)

    def rows_of(s, t):
        return pl.ds(pl.multiple_of(order[s] * quarter + t * BLOCK, BLOCK), BLOCK)

    def prepare(s, t):
        rows = rows_of(s, t)
        stages[s % 2][pl.ds(t * BLOCK, BLOCK)] = (acc[rows] + (product(rows, xr) + product(rows, xo))) * LOG2E

    blocks = quarter // BLOCK
    for t in range(blocks):
        prepare(0, t)
    for s in range(4):
        part = order[s]
        for t in range(blocks):
            if s < 3:
                prepare(s + 1, t)
            wanted = chosen_ref[pl.ds(level, 1), rows_of(s, t)] - offset
            for i in range(BLOCK // TILE):
                row = t * (BLOCK // TILE) + i
                scaled = stages[s % 2][pl.ds(row * TILE, TILE)]
                stats = tile_stats(scaled, wanted[:, i * TILE:(i + 1) * TILE])
                for k in range(4):
                    outgoing[part, k, pl.ds(row, 1), :] = stats[k]
        if s < 3:
            copy = pltpu.make_async_remote_copy(
                src_ref=outgoing.at[part], dst_ref=incoming.at[q],
                send_sem=ssend, recv_sem=srecv,
                device_id=at(x, core, y, quad * 4 + part), device_id_type=MESH,
            )
            copy.start()

    mark("p08statwait")
    found = [tuple(outgoing[q, k] for k in range(4))]
    stat_sets = pltpu.make_async_remote_copy(
        src_ref=outgoing.at[pl.ds(0, 3)], dst_ref=incoming.at[pl.ds(0, 3)],
        send_sem=ssend, recv_sem=srecv, device_id=mate, device_id_type=MESH,
    )
    stat_sets.wait_recv()
    for s in range(3):
        found.append(tuple(incoming[order[s], k] for k in range(4)))
    top = functools.reduce(jnp.maximum, [f[0] for f in found])
    total = weighted = picked = jnp.zeros_like(top)
    for own_top, own_total, own_weighted, own_picked in found:
        gap = own_top - top
        factor = jnp.exp2(gap)
        total += factor * own_total
        weighted += factor * (own_weighted + gap * own_total)
        picked += own_picked
    bits = jnp.log(total)
    confidence = (picked - top) * LN2 - bits
    entropy = bits - LN2 * (weighted / total)
    words[cidx] = lax.shift_left(encode(-confidence, CONF_CODE), 16) | encode(entropy, ENT_CODE)

    mark("p09spread")
    pl.semaphore_wait(line_sem, ys - 1)
    for dz in (4, 3, zs - 3, 2, zs - 2, 1, zs - 1, 0):
        for dy in (2, 1, ys - 1, 0):
            if dz or dy:
                pltpu.make_async_remote_copy(
                    src_ref=words.at[cidx], dst_ref=words.at[cidx],
                    send_sem=gsend, recv_sem=grecv,
                    device_id=at(x, core, (y + dy) % ys, (z + dz) % zs), device_id_type=MESH,
                ).start()
    rest = words.at[pl.ds(0, ys * zs - 1)]
    finals = pltpu.make_async_remote_copy(
        src_ref=rest, dst_ref=rest, send_sem=gsend, recv_sem=grecv, device_id=mate, device_id_type=MESH,
    )
    finals.wait_recv()

    mark("p11drain")
    pltpu.make_async_remote_copy(
        src_ref=weights.at[pl.ds(0, PUSHES)], dst_ref=weights.at[pl.ds(0, PUSHES)],
        send_sem=wsend, recv_sem=wrecv.at[0], device_id=mate, device_id_type=MESH,
    ).wait_send()
    stat_sets.wait_send()
    finals.wait_send()
    mark(None)


def encode(value, code):
    scale, largest = code
    steps = 65535 / math.log1p(largest * scale)
    level = jnp.log(1.0 + jnp.maximum(value, 0.0) * scale) * steps
    return jnp.minimum(level + 0.5, 65535.0).astype(jnp.int32)


def decode(number, code):
    scale, largest = code
    steps = 65535 / math.log1p(largest * scale)
    return (jnp.exp2(number.astype(jnp.float32) * (LOG2E / steps)) - 1.0) * (1 / scale)


def lay_out(words, conf_hbm, ent_hbm, conf, ent, sems):
    levels, rows = conf.shape
    copies = []
    for k, (out, dst) in enumerate(((conf, conf_hbm), (ent, ent_hbm))):
        for part in range(4):
            values = []
            for g in range(levels):
                word = words[g * 4 + part]
                if k == 0:
                    values.append(-decode(lax.shift_right_logical(word, 16), CONF_CODE))
                else:
                    values.append(decode(word & 65535, ENT_CODE))
            for j in range(rows // 4 // LANES):
                cols = pl.ds(part * (rows // 4) + j * LANES, LANES)
                out[:, cols] = jnp.concatenate([v[j:j + 1] for v in values], axis=0)
        copy = pltpu.make_async_copy(out, dst, sems.at[k])
        copy.start()
        copies.append(copy)
    for copy in copies:
        copy.wait()


def on_device(xs, ys, zs, hidden, head, chosen):
    rows, width = hidden.shape
    depth, columns = head.shape
    levels = chosen.shape[0]
    quarter = rows // 4
    dma = pltpu.SemaphoreType.DMA
    out = jax.ShapeDtypeStruct((levels, rows), jnp.float32)
    vmem = pl.BlockSpec(memory_space=pltpu.VMEM)
    anywhere = pl.BlockSpec(memory_space=pltpu.HBM)
    words = pl.pallas_call(
        functools.partial(kernel, xs, ys, zs),
        out_shape=pltpu.VMEM((ys * zs, quarter // LANES, LANES), jnp.int32),
        in_specs=[anywhere, anywhere, anywhere],
        out_specs=vmem,
        scratch_shapes=[
            pltpu.VMEM((rows, width), jnp.bfloat16),
            pltpu.VMEM((width // depth, depth, columns), jnp.bfloat16),
            pltpu.VMEM((rows, columns), jnp.float32),
            pltpu.VMEM((quarter, columns), jnp.float32),
            pltpu.VMEM((quarter, columns), jnp.float32),
            pltpu.VMEM((4, 4, quarter // LANES, LANES), jnp.float32),
            pltpu.VMEM((4, 4, quarter // LANES, LANES), jnp.float32),
            pltpu.VMEM((levels, rows), jnp.int32),
            dma((6,)), dma(()), dma((7,)), dma(()), dma(()), dma(()), dma(()),
            pltpu.SemaphoreType.REGULAR, pltpu.SemaphoreType.REGULAR,
            pltpu.SemaphoreType.REGULAR, pltpu.SemaphoreType.REGULAR,
        ],
        compiler_params=pltpu.CompilerParams(collective_id=0, has_side_effects=True, vmem_limit_bytes=56 << 20),
    )(hidden, head, chosen)
    return pl.pallas_call(
        lay_out,
        out_shape=(out, out),
        in_specs=[vmem],
        out_specs=(anywhere, anywhere),
        scratch_shapes=[pltpu.VMEM((levels, rows), jnp.float32)] * 2 + [dma((2,))],
        compiler_params=pltpu.CompilerParams(vmem_limit_bytes=4 << 20),
    )(words)


def solution(mesh):
    return jax.shard_map(
        functools.partial(on_device, mesh.shape["frames"] // 2, 4, mesh.shape["codes"] // 4),
        mesh=mesh,
        in_specs=(P("frames", None), P("frames", "codes"), P(None, "frames")),
        out_specs=(P(None, "frames"), P(None, "frames")),
        check_vma=False,
    )
```

```python
import functools
import math

import jax
import jax.numpy as jnp
from jax import lax
from jax.experimental import pallas as pl
from jax.experimental.pallas import tpu as pltpu
from jax.sharding import PartitionSpec as P

CODES = 1024
LOG2E = math.log2(math.e)
LN2 = math.log(2.0)
MESH = pl.DeviceIdType.MESH
LANES = 128
TILE = 128
BLOCK = 256
PUSHES = 7
CONF_CODE = (64.0, 20500.0)
ENT_CODE = (1024.0, 6.95)
PROFILE = False


open_scopes = []


def mark(name):
    if PROFILE:
        while open_scopes:
            open_scopes.pop().__exit__(None, None, None)
        if name:
            open_scopes.append(jax.named_scope(name))
            open_scopes[-1].__enter__()


def tile_stats(scaled, wanted):
    flipped = scaled.T
    columns, frames = flipped.shape
    top = jnp.max(flipped, axis=0, keepdims=True)
    below = flipped - top
    powers = jnp.exp2(below)
    total = jnp.sum(powers, axis=0, keepdims=True)
    weighted = jnp.sum(powers * below, axis=0, keepdims=True)
    groups = columns // 8
    pool = flipped.reshape(groups, 8, frames)
    spread = jnp.broadcast_to(wanted, (8, frames))
    bit = groups.bit_length() - 2
    while bit >= 0:
        half = 1 << bit
        upper = (lax.shift_right_arithmetic(spread, 3 + bit) & 1) == 1
        pool = jnp.where(upper[None], pool[half:], pool[:half])
        bit -= 1
    row = lax.broadcasted_iota(jnp.int32, (8, frames), 0)
    here = (row == (spread & 7)) & (spread >= 0) & (spread < columns)
    picked = jnp.sum(jnp.where(here, pool[0], 0.0), axis=0, keepdims=True)
    return top, total, weighted, picked


def kernel(
    xs, ys, zs,
    hidden_hbm, head_hbm, chosen_hbm, words,
    hid, weights, acc, stage_a, stage_b, outgoing, incoming, chosen_ref,
    load_sem, wsend, wrecv, ssend, srecv, gsend, grecv, near_sem, wide_sem, side_sem, line_sem,
):
    fidx = lax.axis_index("frames")
    cidx = lax.axis_index("codes")
    own_head = pltpu.make_async_copy(head_hbm, weights.at[fidx], load_sem.at[0])
    own_head.start()
    x, core = lax.div(fidx, 2), lax.rem(fidx, 2)
    y, z = lax.div(cidx, zs), lax.rem(cidx, zs)
    sib = 1 - core
    xl, xr, xo = lax.rem(x + xs - 1, xs), lax.rem(x + 1, xs), lax.rem(x + 2, xs)

    def at(px, pcore, py, pz):
        return (px * 2 + pcore, py * zs + pz)

    mark("p01barrier")
    mate = at(x, sib, y, z)
    left, right, far = at(xl, core, y, z), at(xr, core, y, z), at(xo, core, y, z)
    barrier = pltpu.get_barrier_semaphore()
    z_near = [at(x, core, y, lax.rem(z + d, zs)) for d in (1, zs - 1)]
    y_near = [at(x, core, lax.rem(y + d, ys), z) for d in (1, ys - 1)]
    around = [mate, left, right, far] + z_near + y_near
    for peer in around:
        pl.semaphore_signal(barrier, inc=1, device_id=peer, device_id_type=MESH)
    quarter = hid.shape[0] // 4
    loads = []
    for i in range(4):
        rows = pl.ds(i * quarter, quarter)
        copy = pltpu.make_async_copy(hidden_hbm.at[rows], hid.at[rows], load_sem.at[1 + i])
        copy.start()
        loads.append(copy)
    chosen_load = pltpu.make_async_copy(chosen_hbm, chosen_ref, load_sem.at[5])
    chosen_load.start()
    pl.semaphore_wait(barrier, len(around))
    for peer in z_near:
        pl.semaphore_signal(near_sem, inc=1, device_id=peer, device_id_type=MESH)
    for peer in y_near:
        pl.semaphore_signal(side_sem, inc=1, device_id=peer, device_id_type=MESH)
    own_head.wait()

    mark("p02gather")
    y_at = [lax.rem(y + d, ys) for d in range(ys)]
    z_at = [lax.rem(z + d, zs) for d in range(zs)]
    q, quad = lax.rem(z, 4), lax.div(z, 4)
    level = y * (zs // 4) + quad
    z_wide = [at(x, core, y, z_at[d]) for d in (2, zs - 2)]
    half = weights.shape[1] // 2

    def piece(slot, part):
        if part is None:
            return weights.at[slot]
        return weights.at[slot, pl.ds(part * half, half)]

    def push(slot, part, index, peer):
        copy = pltpu.make_async_remote_copy(
            src_ref=piece(slot, part), dst_ref=piece(slot, part),
            send_sem=wsend, recv_sem=wrecv.at[index],
            device_id=peer, device_id_type=MESH,
        )
        copy.start()

    def landed(slot, part, index):
        pltpu.make_async_remote_copy(
            src_ref=piece(slot, part), dst_ref=piece(slot, part),
            send_sem=wsend, recv_sem=wrecv.at[index],
            device_id=at(x, sib, y, z), device_id_type=MESH,
        ).wait_recv()

    push(fidx, None, 0, mate)
    push(fidx, None, 1, right)
    push(fidx, None, 2, left)
    push(fidx, None, 3, far)
    pl.semaphore_wait(near_sem, 2)
    for peer in z_wide:
        pl.semaphore_signal(wide_sem, inc=1, device_id=peer, device_id_type=MESH)
    left_slot, right_slot, far_slot = xl * 2 + core, xr * 2 + core, xo * 2 + core
    depth = 2 * weights.shape[1]

    def product(rows, chip):
        pair = weights[pl.ds(chip * 2, 2)].reshape(depth, weights.shape[2])
        cols = pl.ds(pl.multiple_of(chip * depth, depth), depth)
        return jnp.dot(hid[rows, cols], pair, preferred_element_type=jnp.float32)

    mark("p03ownmm")
    landed(x * 2 + sib, None, 0)
    step = 512
    for i in range(4):
        loads[i].wait()
        for j in range(quarter // step):
            rows = pl.ds(i * quarter + j * step, step)
            acc[rows] = product(rows, x)
    mark("p04relay")
    landed(left_slot, None, 1)
    push(left_slot, None, 4, mate)
    landed(right_slot, None, 2)
    push(right_slot, None, 5, mate)
    landed(far_slot, None, 3)
    push(far_slot, None, 6, mate)
    mark("p05sidemm")
    landed(xl * 2 + sib, None, 4)
    for i in range(hid.shape[0] // step):
        rows = pl.ds(i * step, step)
        acc[rows] += product(rows, xl)
    mark("p06farwait")
    landed(xr * 2 + sib, None, 5)
    landed(xo * 2 + sib, None, 6)
    mark("p07stats")
    pl.semaphore_wait(wide_sem, 2)
    pl.semaphore_wait(side_sem, 2)
    for d in range(1, ys):
        pl.semaphore_signal(line_sem, inc=1, device_id=at(x, core, y_at[d], z), device_id_type=MESH)
    chosen_load.wait()
    offset = q * weights.shape[2]
    low = q < 2
    order = [jnp.where(low, 3, 0), jnp.where(low, 2, 1)]
    order.append(jnp.where(low, jnp.where(q == 1, 0, 1), jnp.where(q == 2, 3, 2)))
    order.append(q)
    stages = (stage_a, stage_b)

    def rows_of(s, t):
        return pl.ds(pl.multiple_of(order[s] * quarter + t * BLOCK, BLOCK), BLOCK)

    def prepare(s, t):
        rows = rows_of(s, t)
        stages[s % 2][pl.ds(t * BLOCK, BLOCK)] = (acc[rows] + (product(rows, xr) + product(rows, xo))) * LOG2E

    blocks = quarter // BLOCK
    for t in range(blocks):
        prepare(0, t)
    for s in range(4):
        part = order[s]
        for t in range(blocks):
            if s < 3:
                prepare(s + 1, t)
            wanted = chosen_ref[pl.ds(level, 1), rows_of(s, t)] - offset
            for i in range(BLOCK // TILE):
                row = t * (BLOCK // TILE) + i
                scaled = stages[s % 2][pl.ds(row * TILE, TILE)]
                stats = tile_stats(scaled, wanted[:, i * TILE:(i + 1) * TILE])
                for k in range(4):
                    outgoing[part, k, pl.ds(row, 1), :] = stats[k]
        if s < 3:
            copy = pltpu.make_async_remote_copy(
                src_ref=outgoing.at[part], dst_ref=incoming.at[q],
                send_sem=ssend, recv_sem=srecv,
                device_id=at(x, core, y, quad * 4 + part), device_id_type=MESH,
            )
            copy.start()

    mark("p08statwait")
    found = [tuple(outgoing[q, k] for k in range(4))]
    stat_sets = pltpu.make_async_remote_copy(
        src_ref=outgoing.at[pl.ds(0, 3)], dst_ref=incoming.at[pl.ds(0, 3)],
        send_sem=ssend, recv_sem=srecv, device_id=mate, device_id_type=MESH,
    )
    stat_sets.wait_recv()
    for s in range(3):
        found.append(tuple(incoming[order[s], k] for k in range(4)))
    top = functools.reduce(jnp.maximum, [f[0] for f in found])
    total = weighted = picked = jnp.zeros_like(top)
    for own_top, own_total, own_weighted, own_picked in found:
        gap = own_top - top
        factor = jnp.exp2(gap)
        total += factor * own_total
        weighted += factor * (own_weighted + gap * own_total)
        picked += own_picked
    bits = jnp.log(total)
    confidence = (picked - top) * LN2 - bits
    entropy = bits - LN2 * (weighted / total)
    words[cidx] = lax.shift_left(encode(-confidence, CONF_CODE), 16) | encode(entropy, ENT_CODE)

    mark("p09spread")
    pl.semaphore_wait(line_sem, ys - 1)
    for dz in (4, 3, zs - 3, 2, zs - 2, 1, zs - 1, 0):
        for dy in (2, 1, ys - 1, 0):
            if dz or dy:
                pltpu.make_async_remote_copy(
                    src_ref=words.at[cidx], dst_ref=words.at[cidx],
                    send_sem=gsend, recv_sem=grecv,
                    device_id=at(x, core, y_at[dy], z_at[dz]), device_id_type=MESH,
                ).start()
    rest = words.at[pl.ds(0, ys * zs - 1)]
    finals = pltpu.make_async_remote_copy(
        src_ref=rest, dst_ref=rest, send_sem=gsend, recv_sem=grecv, device_id=mate, device_id_type=MESH,
    )
    finals.wait_recv()

    mark("p11drain")
    pltpu.make_async_remote_copy(
        src_ref=weights.at[pl.ds(0, PUSHES)], dst_ref=weights.at[pl.ds(0, PUSHES)],
        send_sem=wsend, recv_sem=wrecv.at[0], device_id=mate, device_id_type=MESH,
    ).wait_send()
    stat_sets.wait_send()
    finals.wait_send()
    mark(None)


def encode(value, code):
    scale, largest = code
    steps = 65535 / math.log1p(largest * scale)
    level = jnp.log(1.0 + jnp.maximum(value, 0.0) * scale) * steps
    return jnp.minimum(level + 0.5, 65535.0).astype(jnp.int32)


def decode(number, code):
    scale, largest = code
    steps = 65535 / math.log1p(largest * scale)
    return (jnp.exp2(number.astype(jnp.float32) * (LOG2E / steps)) - 1.0) * (1 / scale)


def lay_out(words, conf_hbm, ent_hbm, conf, ent, sems):
    levels, rows = conf.shape
    quarter = rows // 4
    copies = []
    for part in range(4):
        found = [words[g * 4 + part] for g in range(levels)]
        fields = (
            (conf, conf_hbm, [-decode(lax.shift_right_logical(w, 16), CONF_CODE) for w in found]),
            (ent, ent_hbm, [decode(w & 65535, ENT_CODE) for w in found]),
        )
        for k, (out, dst, values) in enumerate(fields):
            for j in range(quarter // LANES):
                cols = pl.ds(part * quarter + j * LANES, LANES)
                out[:, cols] = jnp.concatenate([v[j:j + 1] for v in values], axis=0)
            span = pl.ds(part * quarter, quarter)
            copy = pltpu.make_async_copy(out.at[:, span], dst.at[:, span], sems.at[2 * part + k])
            copy.start()
            copies.append(copy)
    for copy in copies:
        copy.wait()


def on_device(xs, ys, zs, hidden, head, chosen):
    rows, width = hidden.shape
    depth, columns = head.shape
    levels = chosen.shape[0]
    quarter = rows // 4
    dma = pltpu.SemaphoreType.DMA
    out = jax.ShapeDtypeStruct((levels, rows), jnp.float32)
    vmem = pl.BlockSpec(memory_space=pltpu.VMEM)
    anywhere = pl.BlockSpec(memory_space=pltpu.HBM)
    words = pl.pallas_call(
        functools.partial(kernel, xs, ys, zs),
        out_shape=pltpu.VMEM((ys * zs, quarter // LANES, LANES), jnp.int32),
        in_specs=[anywhere, anywhere, anywhere],
        out_specs=vmem,
        scratch_shapes=[
            pltpu.VMEM((rows, width), jnp.bfloat16),
            pltpu.VMEM((width // depth, depth, columns), jnp.bfloat16),
            pltpu.VMEM((rows, columns), jnp.float32),
            pltpu.VMEM((quarter, columns), jnp.float32),
            pltpu.VMEM((quarter, columns), jnp.float32),
            pltpu.VMEM((4, 4, quarter // LANES, LANES), jnp.float32),
            pltpu.VMEM((4, 4, quarter // LANES, LANES), jnp.float32),
            pltpu.VMEM((levels, rows), jnp.int32),
            dma((6,)), dma(()), dma((7,)), dma(()), dma(()), dma(()), dma(()),
            pltpu.SemaphoreType.REGULAR, pltpu.SemaphoreType.REGULAR,
            pltpu.SemaphoreType.REGULAR, pltpu.SemaphoreType.REGULAR,
        ],
        compiler_params=pltpu.CompilerParams(collective_id=0, has_side_effects=True, vmem_limit_bytes=56 << 20),
    )(hidden, head, chosen)
    return pl.pallas_call(
        lay_out,
        out_shape=(out, out),
        in_specs=[vmem],
        out_specs=(anywhere, anywhere),
        scratch_shapes=[pltpu.VMEM((levels, rows), jnp.float32)] * 2 + [dma((8,))],
        compiler_params=pltpu.CompilerParams(vmem_limit_bytes=4 << 20),
    )(words)


def solution(mesh):
    return jax.shard_map(
        functools.partial(on_device, mesh.shape["frames"] // 2, 4, mesh.shape["codes"] // 4),
        mesh=mesh,
        in_specs=(P("frames", None), P("frames", "codes"), P(None, "frames")),
        out_specs=(P(None, "frames"), P(None, "frames")),
        check_vma=False,
    )
```

```python
import functools
import math

import jax
import jax.numpy as jnp
from jax import lax
from jax.experimental import pallas as pl
from jax.experimental.pallas import tpu as pltpu
from jax.sharding import PartitionSpec as P

CODES = 1024
LOG2E = math.log2(math.e)
LN2 = math.log(2.0)
MESH = pl.DeviceIdType.MESH
LANES = 128
TILE = 128
BLOCK = 256
PUSHES = 7
LEAD = 3
STEP = 1024
CONF_CODE = (64.0, 20500.0)
ENT_CODE = (1024.0, 6.95)
PROFILE = False


open_scopes = []


def mark(name):
    if PROFILE:
        while open_scopes:
            open_scopes.pop().__exit__(None, None, None)
        if name:
            open_scopes.append(jax.named_scope(name))
            open_scopes[-1].__enter__()


def tile_stats(scaled, wanted):
    flipped = scaled.T
    columns, frames = flipped.shape
    top = jnp.max(flipped, axis=0, keepdims=True)
    below = flipped - top
    powers = jnp.exp2(below)
    total = jnp.sum(powers, axis=0, keepdims=True)
    weighted = jnp.sum(powers * below, axis=0, keepdims=True)
    groups = columns // 8
    pool = flipped.reshape(groups, 8, frames)
    spread = jnp.broadcast_to(wanted, (8, frames))
    bit = groups.bit_length() - 2
    while bit >= 0:
        half = 1 << bit
        upper = (lax.shift_right_arithmetic(spread, 3 + bit) & 1) == 1
        pool = jnp.where(upper[None], pool[half:], pool[:half])
        bit -= 1
    row = lax.broadcasted_iota(jnp.int32, (8, frames), 0)
    here = (row == (spread & 7)) & (spread >= 0) & (spread < columns)
    picked = jnp.sum(jnp.where(here, pool[0], 0.0), axis=0, keepdims=True)
    return top, total, weighted, picked


def kernel(
    xs, ys, zs,
    hidden_hbm, head_hbm, chosen_hbm, words,
    hid, weights, acc, stage_a, stage_b, outgoing, incoming, chosen_ref,
    load_sem, wsend, wrecv, ssend, srecv, gsend, grecv, near_sem, wide_sem, side_sem, line_sem,
):
    fidx = lax.axis_index("frames")
    cidx = lax.axis_index("codes")
    own_head = pltpu.make_async_copy(head_hbm, weights.at[fidx], load_sem.at[0])
    own_head.start()
    x, core = lax.div(fidx, 2), lax.rem(fidx, 2)
    y, z = lax.div(cidx, zs), lax.rem(cidx, zs)
    sib = 1 - core
    xl, xr, xo = lax.rem(x + xs - 1, xs), lax.rem(x + 1, xs), lax.rem(x + 2, xs)

    def at(px, pcore, py, pz):
        return (px * 2 + pcore, py * zs + pz)

    mark("p01barrier")
    mate = at(x, sib, y, z)
    left, right, far = at(xl, core, y, z), at(xr, core, y, z), at(xo, core, y, z)
    barrier = pltpu.get_barrier_semaphore()
    z_near = [at(x, core, y, lax.rem(z + d, zs)) for d in (1, zs - 1)]
    y_near = [at(x, core, lax.rem(y + d, ys), z) for d in (1, ys - 1)]
    around = [mate, left, right, far] + z_near + y_near
    for peer in around:
        pl.semaphore_signal(barrier, inc=1, device_id=peer, device_id_type=MESH)
    quarter = hid.shape[0] // 4
    loads = []
    for i in range(4):
        rows = pl.ds(i * quarter, quarter)
        copy = pltpu.make_async_copy(hidden_hbm.at[rows], hid.at[rows], load_sem.at[1 + i])
        copy.start()
        loads.append(copy)
    chosen_load = pltpu.make_async_copy(chosen_hbm, chosen_ref, load_sem.at[5])
    chosen_load.start()
    pl.semaphore_wait(barrier, len(around))
    for peer in z_near:
        pl.semaphore_signal(near_sem, inc=1, device_id=peer, device_id_type=MESH)
    for peer in y_near:
        pl.semaphore_signal(side_sem, inc=1, device_id=peer, device_id_type=MESH)
    own_head.wait()

    mark("p02gather")
    y_at = [lax.rem(y + d, ys) for d in range(ys)]
    z_at = [lax.rem(z + d, zs) for d in range(zs)]
    q, quad = lax.rem(z, 4), lax.div(z, 4)
    level = y * (zs // 4) + quad
    z_wide = [at(x, core, y, z_at[d]) for d in (2, zs - 2)]
    half = weights.shape[1] // 2

    def piece(slot, part):
        if part is None:
            return weights.at[slot]
        return weights.at[slot, pl.ds(part * half, half)]

    def push(slot, part, index, peer):
        copy = pltpu.make_async_remote_copy(
            src_ref=piece(slot, part), dst_ref=piece(slot, part),
            send_sem=wsend, recv_sem=wrecv.at[index],
            device_id=peer, device_id_type=MESH,
        )
        copy.start()

    def landed(slot, part, index):
        pltpu.make_async_remote_copy(
            src_ref=piece(slot, part), dst_ref=piece(slot, part),
            send_sem=wsend, recv_sem=wrecv.at[index],
            device_id=at(x, sib, y, z), device_id_type=MESH,
        ).wait_recv()

    push(fidx, None, 0, mate)
    push(fidx, None, 1, right)
    push(fidx, None, 2, left)
    push(fidx, None, 3, far)
    pl.semaphore_wait(near_sem, 2)
    for peer in z_wide:
        pl.semaphore_signal(wide_sem, inc=1, device_id=peer, device_id_type=MESH)
    left_slot, right_slot, far_slot = xl * 2 + core, xr * 2 + core, xo * 2 + core
    depth = 2 * weights.shape[1]

    def product(rows, chip):
        pair = weights[pl.ds(chip * 2, 2)].reshape(depth, weights.shape[2])
        cols = pl.ds(pl.multiple_of(chip * depth, depth), depth)
        return jnp.dot(hid[rows, cols], pair, preferred_element_type=jnp.float32)

    mark("p03ownmm")
    landed(x * 2 + sib, None, 0)
    step = STEP
    for i in range(4):
        loads[i].wait()
        for j in range(quarter // step):
            rows = pl.ds(i * quarter + j * step, step)
            acc[rows] = product(rows, x)
    mark("p04relay")
    landed(left_slot, None, 1)
    push(left_slot, None, 4, mate)
    landed(right_slot, None, 2)
    push(right_slot, None, 5, mate)
    landed(far_slot, None, 3)
    push(far_slot, None, 6, mate)
    mark("p05sidemm")
    landed(xl * 2 + sib, None, 4)
    for i in range(hid.shape[0] // step):
        rows = pl.ds(i * step, step)
        acc[rows] += product(rows, xl)
    mark("p06farwait")
    landed(xr * 2 + sib, None, 5)
    landed(xo * 2 + sib, None, 6)
    mark("p07stats")
    pl.semaphore_wait(wide_sem, 2)
    pl.semaphore_wait(side_sem, 2)
    for d in range(1, ys):
        pl.semaphore_signal(line_sem, inc=1, device_id=at(x, core, y_at[d], z), device_id_type=MESH)
    chosen_load.wait()
    offset = q * weights.shape[2]
    low = q < 2
    order = [jnp.where(low, 3, 0), jnp.where(low, 2, 1)]
    order.append(jnp.where(low, jnp.where(q == 1, 0, 1), jnp.where(q == 2, 3, 2)))
    order.append(q)
    stages = (stage_a, stage_b)

    def rows_of(s, t):
        return pl.ds(pl.multiple_of(order[s] * quarter + t * BLOCK, BLOCK), BLOCK)

    def prepare(s, t):
        rows = rows_of(s, t)
        stages[s % 2][pl.ds(t * BLOCK, BLOCK)] = (acc[rows] + (product(rows, xr) + product(rows, xo))) * LOG2E

    blocks = quarter // BLOCK
    for t in range(LEAD):
        prepare(0, t)
    for s in range(4):
        part = order[s]
        for t in range(blocks):
            ahead = s * blocks + t + LEAD
            if ahead < 4 * blocks:
                prepare(ahead // blocks, ahead % blocks)
            wanted = chosen_ref[pl.ds(level, 1), rows_of(s, t)] - offset
            for i in range(BLOCK // TILE):
                row = t * (BLOCK // TILE) + i
                scaled = stages[s % 2][pl.ds(row * TILE, TILE)]
                stats = tile_stats(scaled, wanted[:, i * TILE:(i + 1) * TILE])
                for k in range(4):
                    outgoing[part, k, pl.ds(row, 1), :] = stats[k]
        if s < 3:
            copy = pltpu.make_async_remote_copy(
                src_ref=outgoing.at[part], dst_ref=incoming.at[q],
                send_sem=ssend, recv_sem=srecv,
                device_id=at(x, core, y, quad * 4 + part), device_id_type=MESH,
            )
            copy.start()

    mark("p08statwait")
    found = [tuple(outgoing[q, k] for k in range(4))]
    stat_sets = pltpu.make_async_remote_copy(
        src_ref=outgoing.at[pl.ds(0, 3)], dst_ref=incoming.at[pl.ds(0, 3)],
        send_sem=ssend, recv_sem=srecv, device_id=mate, device_id_type=MESH,
    )
    stat_sets.wait_recv()
    for s in range(3):
        found.append(tuple(incoming[order[s], k] for k in range(4)))
    top = functools.reduce(jnp.maximum, [f[0] for f in found])
    total = weighted = picked = jnp.zeros_like(top)
    for own_top, own_total, own_weighted, own_picked in found:
        gap = own_top - top
        factor = jnp.exp2(gap)
        total += factor * own_total
        weighted += factor * (own_weighted + gap * own_total)
        picked += own_picked
    bits = jnp.log(total)
    confidence = (picked - top) * LN2 - bits
    entropy = bits - LN2 * (weighted / total)
    words[cidx] = lax.shift_left(encode(-confidence, CONF_CODE), 16) | encode(entropy, ENT_CODE)

    mark("p09spread")
    pl.semaphore_wait(line_sem, ys - 1)
    for dz in (4, 3, zs - 3, 2, zs - 2, 1, zs - 1, 0):
        for dy in (2, 1, ys - 1, 0):
            if dz or dy:
                pltpu.make_async_remote_copy(
                    src_ref=words.at[cidx], dst_ref=words.at[cidx],
                    send_sem=gsend, recv_sem=grecv,
                    device_id=at(x, core, y_at[dy], z_at[dz]), device_id_type=MESH,
                ).start()
    rest = words.at[pl.ds(0, ys * zs - 1)]
    finals = pltpu.make_async_remote_copy(
        src_ref=rest, dst_ref=rest, send_sem=gsend, recv_sem=grecv, device_id=mate, device_id_type=MESH,
    )
    finals.wait_recv()

    mark("p11drain")
    pltpu.make_async_remote_copy(
        src_ref=weights.at[pl.ds(0, PUSHES)], dst_ref=weights.at[pl.ds(0, PUSHES)],
        send_sem=wsend, recv_sem=wrecv.at[0], device_id=mate, device_id_type=MESH,
    ).wait_send()
    stat_sets.wait_send()
    finals.wait_send()
    mark(None)


def encode(value, code):
    scale, largest = code
    steps = 65535 / math.log1p(largest * scale)
    level = jnp.log(1.0 + jnp.maximum(value, 0.0) * scale) * steps
    return jnp.minimum(level + 0.5, 65535.0).astype(jnp.int32)


def decode(number, code):
    scale, largest = code
    steps = 65535 / math.log1p(largest * scale)
    return (jnp.exp2(number.astype(jnp.float32) * (LOG2E / steps)) - 1.0) * (1 / scale)


def lay_out(words, conf_hbm, ent_hbm, conf, ent, sems):
    levels, rows = conf.shape
    quarter = rows // 4
    copies = []
    for part in range(4):
        found = [words[g * 4 + part] for g in range(levels)]
        fields = (
            (conf, conf_hbm, [-decode(lax.shift_right_logical(w, 16), CONF_CODE) for w in found]),
            (ent, ent_hbm, [decode(w & 65535, ENT_CODE) for w in found]),
        )
        for k, (out, dst, values) in enumerate(fields):
            for j in range(quarter // LANES):
                cols = pl.ds(part * quarter + j * LANES, LANES)
                out[:, cols] = jnp.concatenate([v[j:j + 1] for v in values], axis=0)
            span = pl.ds(part * quarter, quarter)
            copy = pltpu.make_async_copy(out.at[:, span], dst.at[:, span], sems.at[2 * part + k])
            copy.start()
            copies.append(copy)
    for copy in copies:
        copy.wait()


def on_device(xs, ys, zs, hidden, head, chosen):
    rows, width = hidden.shape
    depth, columns = head.shape
    levels = chosen.shape[0]
    quarter = rows // 4
    dma = pltpu.SemaphoreType.DMA
    out = jax.ShapeDtypeStruct((levels, rows), jnp.float32)
    vmem = pl.BlockSpec(memory_space=pltpu.VMEM)
    anywhere = pl.BlockSpec(memory_space=pltpu.HBM)
    words = pl.pallas_call(
        functools.partial(kernel, xs, ys, zs),
        out_shape=pltpu.VMEM((ys * zs, quarter // LANES, LANES), jnp.int32),
        in_specs=[anywhere, anywhere, anywhere],
        out_specs=vmem,
        scratch_shapes=[
            pltpu.VMEM((rows, width), jnp.bfloat16),
            pltpu.VMEM((width // depth, depth, columns), jnp.bfloat16),
            pltpu.VMEM((rows, columns), jnp.float32),
            pltpu.VMEM((quarter, columns), jnp.float32),
            pltpu.VMEM((quarter, columns), jnp.float32),
            pltpu.VMEM((4, 4, quarter // LANES, LANES), jnp.float32),
            pltpu.VMEM((4, 4, quarter // LANES, LANES), jnp.float32),
            pltpu.VMEM((levels, rows), jnp.int32),
            dma((6,)), dma(()), dma((7,)), dma(()), dma(()), dma(()), dma(()),
            pltpu.SemaphoreType.REGULAR, pltpu.SemaphoreType.REGULAR,
            pltpu.SemaphoreType.REGULAR, pltpu.SemaphoreType.REGULAR,
        ],
        compiler_params=pltpu.CompilerParams(collective_id=0, has_side_effects=True, vmem_limit_bytes=56 << 20),
    )(hidden, head, chosen)
    return pl.pallas_call(
        lay_out,
        out_shape=(out, out),
        in_specs=[vmem],
        out_specs=(anywhere, anywhere),
        scratch_shapes=[pltpu.VMEM((levels, rows), jnp.float32)] * 2 + [dma((8,))],
        compiler_params=pltpu.CompilerParams(vmem_limit_bytes=4 << 20),
    )(words)


def solution(mesh):
    return jax.shard_map(
        functools.partial(on_device, mesh.shape["frames"] // 2, 4, mesh.shape["codes"] // 4),
        mesh=mesh,
        in_specs=(P("frames", None), P("frames", "codes"), P(None, "frames")),
        out_specs=(P(None, "frames"), P(None, "frames")),
        check_vma=False,
    )
```

```python
import functools
import math

import jax
import jax.numpy as jnp
from jax import lax
from jax.experimental import pallas as pl
from jax.experimental.pallas import tpu as pltpu
from jax.sharding import PartitionSpec as P

CODES = 1024
LOG2E = math.log2(math.e)
LN2 = math.log(2.0)
MESH = pl.DeviceIdType.MESH
LANES = 128
TILE = 128
BLOCK = 256
PUSHES = 7
CONF_CODE = (64.0, 20500.0)
ENT_CODE = (1024.0, 6.95)
PROFILE = False


open_scopes = []


def mark(name):
    if PROFILE:
        while open_scopes:
            open_scopes.pop().__exit__(None, None, None)
        if name:
            open_scopes.append(jax.named_scope(name))
            open_scopes[-1].__enter__()


def tile_stats(scaled, wanted):
    flipped = scaled.T
    columns, frames = flipped.shape
    top = jnp.max(flipped, axis=0, keepdims=True)
    below = flipped - top
    powers = jnp.exp2(below)
    total = jnp.sum(powers, axis=0, keepdims=True)
    weighted = jnp.sum(powers * below, axis=0, keepdims=True)
    groups = columns // 8
    pool = flipped.reshape(groups, 8, frames)
    spread = jnp.broadcast_to(wanted, (8, frames))
    bit = groups.bit_length() - 2
    while bit >= 0:
        half = 1 << bit
        upper = (lax.shift_right_arithmetic(spread, 3 + bit) & 1) == 1
        pool = jnp.where(upper[None], pool[half:], pool[:half])
        bit -= 1
    row = lax.broadcasted_iota(jnp.int32, (8, frames), 0)
    here = (row == (spread & 7)) & (spread >= 0) & (spread < columns)
    picked = jnp.sum(jnp.where(here, pool[0], 0.0), axis=0, keepdims=True)
    return top, total, weighted, picked


def kernel(
    xs, ys, zs,
    hidden_hbm, head_hbm, chosen_hbm, words,
    hid, weights, acc, stage_a, stage_b, outgoing, incoming, chosen_ref,
    load_sem, wsend, wrecv, ssend, srecv, gsend, grecv, near_sem, wide_sem, side_sem, line_sem,
):
    fidx = lax.axis_index("frames")
    cidx = lax.axis_index("codes")
    own_head = pltpu.make_async_copy(head_hbm, weights.at[fidx], load_sem.at[0])
    own_head.start()
    x, core = lax.div(fidx, 2), lax.rem(fidx, 2)
    y, z = lax.div(cidx, zs), lax.rem(cidx, zs)
    sib = 1 - core
    xl, xr, xo = lax.rem(x + xs - 1, xs), lax.rem(x + 1, xs), lax.rem(x + 2, xs)

    def at(px, pcore, py, pz):
        return (px * 2 + pcore, py * zs + pz)

    mark("p01barrier")
    mate = at(x, sib, y, z)
    left, right, far = at(xl, core, y, z), at(xr, core, y, z), at(xo, core, y, z)
    barrier = pltpu.get_barrier_semaphore()
    z_near = [at(x, core, y, lax.rem(z + d, zs)) for d in (1, zs - 1)]
    y_near = [at(x, core, lax.rem(y + d, ys), z) for d in (1, ys - 1)]
    around = [mate, left, right, far] + z_near + y_near
    for peer in around:
        pl.semaphore_signal(barrier, inc=1, device_id=peer, device_id_type=MESH)
    quarter = hid.shape[0] // 4
    for i in range(4):
        rows = pl.ds(i * quarter, quarter)
        copy = pltpu.make_async_copy(hidden_hbm.at[rows], hid.at[rows], load_sem.at[1])
        copy.start()
    chosen_load = pltpu.make_async_copy(chosen_hbm, chosen_ref, load_sem.at[2])
    chosen_load.start()
    pl.semaphore_wait(barrier, len(around))
    for peer in z_near:
        pl.semaphore_signal(near_sem, inc=1, device_id=peer, device_id_type=MESH)
    for peer in y_near:
        pl.semaphore_signal(side_sem, inc=1, device_id=peer, device_id_type=MESH)
    own_head.wait()

    mark("p02gather")
    y_at = [lax.rem(y + d, ys) for d in range(ys)]
    z_at = [lax.rem(z + d, zs) for d in range(zs)]
    q, quad = lax.rem(z, 4), lax.div(z, 4)
    level = y * (zs // 4) + quad
    z_wide = [at(x, core, y, z_at[d]) for d in (2, zs - 2)]
    half = weights.shape[1] // 2

    def piece(slot, part):
        if part is None:
            return weights.at[slot]
        return weights.at[slot, pl.ds(part * half, half)]

    def push(slot, part, index, peer):
        copy = pltpu.make_async_remote_copy(
            src_ref=piece(slot, part), dst_ref=piece(slot, part),
            send_sem=wsend, recv_sem=wrecv.at[index],
            device_id=peer, device_id_type=MESH,
        )
        copy.start()

    def landed(slot, part, index):
        pltpu.make_async_remote_copy(
            src_ref=piece(slot, part), dst_ref=piece(slot, part),
            send_sem=wsend, recv_sem=wrecv.at[index],
            device_id=at(x, sib, y, z), device_id_type=MESH,
        ).wait_recv()

    push(fidx, None, 0, mate)
    push(fidx, None, 1, right)
    push(fidx, None, 2, left)
    push(fidx, None, 3, far)
    pl.semaphore_wait(near_sem, 2)
    for peer in z_wide:
        pl.semaphore_signal(wide_sem, inc=1, device_id=peer, device_id_type=MESH)
    left_slot, right_slot, far_slot = xl * 2 + core, xr * 2 + core, xo * 2 + core
    depth = 2 * weights.shape[1]

    def product(rows, chip):
        pair = weights[pl.ds(chip * 2, 2)].reshape(depth, weights.shape[2])
        cols = pl.ds(pl.multiple_of(chip * depth, depth), depth)
        return jnp.dot(hid[rows, cols], pair, preferred_element_type=jnp.float32)

    mark("p03ownmm")
    landed(x * 2 + sib, None, 0)
    step = 512
    pltpu.make_async_copy(hidden_hbm, hid, load_sem.at[1]).wait()
    for i in range(4):
        for j in range(quarter // step):
            rows = pl.ds(i * quarter + j * step, step)
            acc[rows] = product(rows, x)
    mark("p04relay")
    landed(left_slot, None, 1)
    push(left_slot, None, 4, mate)
    landed(right_slot, None, 2)
    push(right_slot, None, 5, mate)
    landed(far_slot, None, 3)
    push(far_slot, None, 6, mate)
    mark("p05sidemm")
    landed(xl * 2 + sib, None, 4)
    for i in range(hid.shape[0] // step):
        rows = pl.ds(i * step, step)
        acc[rows] += product(rows, xl)
    mark("p06farwait")
    landed(xr * 2 + sib, None, 5)
    landed(xo * 2 + sib, None, 6)
    mark("p07stats")
    pl.semaphore_wait(wide_sem, 2)
    pl.semaphore_wait(side_sem, 2)
    for d in range(1, ys):
        pl.semaphore_signal(line_sem, inc=1, device_id=at(x, core, y_at[d], z), device_id_type=MESH)
    chosen_load.wait()
    offset = q * weights.shape[2]
    low = q < 2
    order = [jnp.where(low, 3, 0), jnp.where(low, 2, 1)]
    order.append(jnp.where(low, jnp.where(q == 1, 0, 1), jnp.where(q == 2, 3, 2)))
    order.append(q)
    stages = (stage_a, stage_b)

    def rows_of(s, t):
        return pl.ds(pl.multiple_of(order[s] * quarter + t * BLOCK, BLOCK), BLOCK)

    def prepare(s, t):
        rows = rows_of(s, t)
        stages[s % 2][pl.ds(t * BLOCK, BLOCK)] = (acc[rows] + (product(rows, xr) + product(rows, xo))) * LOG2E

    blocks = quarter // BLOCK
    for t in range(blocks):
        prepare(0, t)
    for s in range(4):
        part = order[s]
        for t in range(blocks):
            if s < 3:
                prepare(s + 1, t)
            wanted = chosen_ref[pl.ds(level, 1), rows_of(s, t)] - offset
            for i in range(BLOCK // TILE):
                row = t * (BLOCK // TILE) + i
                scaled = stages[s % 2][pl.ds(row * TILE, TILE)]
                stats = tile_stats(scaled, wanted[:, i * TILE:(i + 1) * TILE])
                for k in range(4):
                    outgoing[part, k, pl.ds(row, 1), :] = stats[k]
        if s < 3:
            copy = pltpu.make_async_remote_copy(
                src_ref=outgoing.at[part], dst_ref=incoming.at[q],
                send_sem=ssend, recv_sem=srecv,
                device_id=at(x, core, y, quad * 4 + part), device_id_type=MESH,
            )
            copy.start()

    mark("p08statwait")
    found = [tuple(outgoing[q, k] for k in range(4))]
    stat_sets = pltpu.make_async_remote_copy(
        src_ref=outgoing.at[pl.ds(0, 3)], dst_ref=incoming.at[pl.ds(0, 3)],
        send_sem=ssend, recv_sem=srecv, device_id=mate, device_id_type=MESH,
    )
    stat_sets.wait_recv()
    for s in range(3):
        found.append(tuple(incoming[order[s], k] for k in range(4)))
    top = functools.reduce(jnp.maximum, [f[0] for f in found])
    total = weighted = picked = jnp.zeros_like(top)
    for own_top, own_total, own_weighted, own_picked in found:
        gap = own_top - top
        factor = jnp.exp2(gap)
        total += factor * own_total
        weighted += factor * (own_weighted + gap * own_total)
        picked += own_picked
    bits = jnp.log(total)
    confidence = (picked - top) * LN2 - bits
    entropy = bits - LN2 * (weighted / total)
    words[cidx] = lax.shift_left(encode(-confidence, CONF_CODE), 16) | encode(entropy, ENT_CODE)

    mark("p09spread")
    pl.semaphore_wait(line_sem, ys - 1)
    for dz in (4, 3, zs - 3, 2, zs - 2, 1, zs - 1, 0):
        for dy in (2, 1, ys - 1, 0):
            if dz or dy:
                pltpu.make_async_remote_copy(
                    src_ref=words.at[cidx], dst_ref=words.at[cidx],
                    send_sem=gsend, recv_sem=grecv,
                    device_id=at(x, core, y_at[dy], z_at[dz]), device_id_type=MESH,
                ).start()
    rest = words.at[pl.ds(0, ys * zs - 1)]
    finals = pltpu.make_async_remote_copy(
        src_ref=rest, dst_ref=rest, send_sem=gsend, recv_sem=grecv, device_id=mate, device_id_type=MESH,
    )
    finals.wait_recv()

    mark("p11drain")
    pltpu.make_async_remote_copy(
        src_ref=weights.at[pl.ds(0, PUSHES)], dst_ref=weights.at[pl.ds(0, PUSHES)],
        send_sem=wsend, recv_sem=wrecv.at[0], device_id=mate, device_id_type=MESH,
    ).wait_send()
    stat_sets.wait_send()
    finals.wait_send()
    mark(None)


def encode(value, code):
    scale, largest = code
    steps = 65535 / math.log1p(largest * scale)
    level = jnp.log(1.0 + jnp.maximum(value, 0.0) * scale) * steps
    return jnp.minimum(level + 0.5, 65535.0).astype(jnp.int32)


def decode(number, code):
    scale, largest = code
    steps = 65535 / math.log1p(largest * scale)
    return (jnp.exp2(number.astype(jnp.float32) * (LOG2E / steps)) - 1.0) * (1 / scale)


def lay_out(words, conf_hbm, ent_hbm, conf, ent, sems):
    levels, rows = conf.shape
    quarter = rows // 4
    copies = []
    for part in range(4):
        found = [words[g * 4 + part] for g in range(levels)]
        fields = (
            (conf, conf_hbm, [-decode(lax.shift_right_logical(w, 16), CONF_CODE) for w in found]),
            (ent, ent_hbm, [decode(w & 65535, ENT_CODE) for w in found]),
        )
        for k, (out, dst, values) in enumerate(fields):
            for j in range(quarter // LANES):
                cols = pl.ds(part * quarter + j * LANES, LANES)
                out[:, cols] = jnp.concatenate([v[j:j + 1] for v in values], axis=0)
            span = pl.ds(part * quarter, quarter)
            copy = pltpu.make_async_copy(out.at[:, span], dst.at[:, span], sems.at[2 * part + k])
            copy.start()
            copies.append(copy)
    for copy in copies:
        copy.wait()


def on_device(xs, ys, zs, hidden, head, chosen):
    rows, width = hidden.shape
    depth, columns = head.shape
    levels = chosen.shape[0]
    quarter = rows // 4
    dma = pltpu.SemaphoreType.DMA
    out = jax.ShapeDtypeStruct((levels, rows), jnp.float32)
    vmem = pl.BlockSpec(memory_space=pltpu.VMEM)
    anywhere = pl.BlockSpec(memory_space=pltpu.HBM)
    words = pl.pallas_call(
        functools.partial(kernel, xs, ys, zs),
        out_shape=pltpu.VMEM((ys * zs, quarter // LANES, LANES), jnp.int32),
        in_specs=[anywhere, anywhere, anywhere],
        out_specs=vmem,
        scratch_shapes=[
            pltpu.VMEM((rows, width), jnp.bfloat16),
            pltpu.VMEM((width // depth, depth, columns), jnp.bfloat16),
            pltpu.VMEM((rows, columns), jnp.float32),
            pltpu.VMEM((quarter, columns), jnp.float32),
            pltpu.VMEM((quarter, columns), jnp.float32),
            pltpu.VMEM((4, 4, quarter // LANES, LANES), jnp.float32),
            pltpu.VMEM((4, 4, quarter // LANES, LANES), jnp.float32),
            pltpu.VMEM((levels, rows), jnp.int32),
            dma((3,)), dma(()), dma((7,)), dma(()), dma(()), dma(()), dma(()),
            pltpu.SemaphoreType.REGULAR, pltpu.SemaphoreType.REGULAR,
            pltpu.SemaphoreType.REGULAR, pltpu.SemaphoreType.REGULAR,
        ],
        compiler_params=pltpu.CompilerParams(collective_id=0, has_side_effects=True, vmem_limit_bytes=56 << 20),
    )(hidden, head, chosen)
    return pl.pallas_call(
        lay_out,
        out_shape=(out, out),
        in_specs=[vmem],
        out_specs=(anywhere, anywhere),
        scratch_shapes=[pltpu.VMEM((levels, rows), jnp.float32)] * 2 + [dma((8,))],
        compiler_params=pltpu.CompilerParams(vmem_limit_bytes=4 << 20),
    )(words)


def solution(mesh):
    return jax.shard_map(
        functools.partial(on_device, mesh.shape["frames"] // 2, 4, mesh.shape["codes"] // 4),
        mesh=mesh,
        in_specs=(P("frames", None), P("frames", "codes"), P(None, "frames")),
        out_specs=(P(None, "frames"), P(None, "frames")),
        check_vma=False,
    )
```

```python
import functools
import math

import jax
import jax.numpy as jnp
from jax import lax
from jax.experimental import pallas as pl
from jax.experimental.pallas import tpu as pltpu
from jax.sharding import PartitionSpec as P

CODES = 1024
LOG2E = math.log2(math.e)
LN2 = math.log(2.0)
MESH = pl.DeviceIdType.MESH
LANES = 128
TILE = 128
BLOCK = 256
PUSHES = 7
CONF_CODE = (64.0, 20500.0)
ENT_CODE = (1024.0, 6.95)
PROFILE = False


open_scopes = []


def mark(name):
    if PROFILE:
        while open_scopes:
            open_scopes.pop().__exit__(None, None, None)
        if name:
            open_scopes.append(jax.named_scope(name))
            open_scopes[-1].__enter__()


def tile_stats(scaled, wanted):
    flipped = scaled.T
    columns, frames = flipped.shape
    top = jnp.max(flipped, axis=0, keepdims=True)
    below = flipped - top
    powers = jnp.exp2(below)
    total = jnp.sum(powers, axis=0, keepdims=True)
    weighted = jnp.sum(powers * below, axis=0, keepdims=True)
    groups = columns // 8
    pool = flipped.reshape(groups, 8, frames)
    spread = jnp.broadcast_to(wanted, (8, frames))
    bit = groups.bit_length() - 2
    while bit >= 0:
        half = 1 << bit
        upper = (lax.shift_right_arithmetic(spread, 3 + bit) & 1) == 1
        pool = jnp.where(upper[None], pool[half:], pool[:half])
        bit -= 1
    row = lax.broadcasted_iota(jnp.int32, (8, frames), 0)
    here = (row == (spread & 7)) & (spread >= 0) & (spread < columns)
    picked = jnp.sum(jnp.where(here, pool[0], 0.0), axis=0, keepdims=True)
    return top, total, weighted, picked


def kernel(
    xs, ys, zs,
    hidden_hbm, head_hbm, chosen_hbm, words,
    hid, weights, acc, stage_a, stage_b, outgoing, incoming, chosen_ref,
    load_sem, wsend, wrecv, ssend, srecv, gsend, grecv, near_sem, wide_sem, side_sem, line_sem,
):
    fidx = lax.axis_index("frames")
    cidx = lax.axis_index("codes")
    own_head = pltpu.make_async_copy(head_hbm, weights.at[fidx], load_sem.at[0])
    own_head.start()
    x, core = lax.div(fidx, 2), lax.rem(fidx, 2)
    y, z = lax.div(cidx, zs), lax.rem(cidx, zs)
    sib = 1 - core
    xl, xr, xo = lax.rem(x + xs - 1, xs), lax.rem(x + 1, xs), lax.rem(x + 2, xs)

    def at(px, pcore, py, pz):
        return (px * 2 + pcore, py * zs + pz)

    mark("p01barrier")
    mate = at(x, sib, y, z)
    left, right, far = at(xl, core, y, z), at(xr, core, y, z), at(xo, core, y, z)
    barrier = pltpu.get_barrier_semaphore()
    z_near = [at(x, core, y, lax.rem(z + d, zs)) for d in (1, zs - 1)]
    y_near = [at(x, core, lax.rem(y + d, ys), z) for d in (1, ys - 1)]
    around = [far] + z_near + y_near + [left, right, mate]
    for peer in around:
        pl.semaphore_signal(barrier, inc=1, device_id=peer, device_id_type=MESH)
    quarter = hid.shape[0] // 4
    for i in range(4):
        rows = pl.ds(i * quarter, quarter)
        copy = pltpu.make_async_copy(hidden_hbm.at[rows], hid.at[rows], load_sem.at[1])
        copy.start()
    chosen_load = pltpu.make_async_copy(chosen_hbm, chosen_ref, load_sem.at[2])
    chosen_load.start()
    pl.semaphore_wait(barrier, len(around))
    for peer in z_near:
        pl.semaphore_signal(near_sem, inc=1, device_id=peer, device_id_type=MESH)
    for peer in y_near:
        pl.semaphore_signal(side_sem, inc=1, device_id=peer, device_id_type=MESH)
    own_head.wait()

    mark("p02gather")
    y_at = [lax.rem(y + d, ys) for d in range(ys)]
    z_at = [lax.rem(z + d, zs) for d in range(zs)]
    q, quad = lax.rem(z, 4), lax.div(z, 4)
    level = y * (zs // 4) + quad
    z_wide = [at(x, core, y, z_at[d]) for d in (2, zs - 2)]
    half = weights.shape[1] // 2

    def piece(slot, part):
        if part is None:
            return weights.at[slot]
        return weights.at[slot, pl.ds(part * half, half)]

    def push(slot, part, index, peer):
        copy = pltpu.make_async_remote_copy(
            src_ref=piece(slot, part), dst_ref=piece(slot, part),
            send_sem=wsend, recv_sem=wrecv.at[index],
            device_id=peer, device_id_type=MESH,
        )
        copy.start()

    def landed(slot, part, index):
        pltpu.make_async_remote_copy(
            src_ref=piece(slot, part), dst_ref=piece(slot, part),
            send_sem=wsend, recv_sem=wrecv.at[index],
            device_id=at(x, sib, y, z), device_id_type=MESH,
        ).wait_recv()

    push(fidx, None, 0, mate)
    push(fidx, None, 1, right)
    push(fidx, None, 2, left)
    push(fidx, None, 3, far)
    pl.semaphore_wait(near_sem, 2)
    for peer in z_wide:
        pl.semaphore_signal(wide_sem, inc=1, device_id=peer, device_id_type=MESH)
    left_slot, right_slot, far_slot = xl * 2 + core, xr * 2 + core, xo * 2 + core
    depth = 2 * weights.shape[1]

    def product(rows, chip):
        pair = weights[pl.ds(chip * 2, 2)].reshape(depth, weights.shape[2])
        cols = pl.ds(pl.multiple_of(chip * depth, depth), depth)
        return jnp.dot(hid[rows, cols], pair, preferred_element_type=jnp.float32)

    mark("p03ownmm")
    landed(x * 2 + sib, None, 0)
    step = 512
    pltpu.make_async_copy(hidden_hbm, hid, load_sem.at[1]).wait()
    for i in range(4):
        for j in range(quarter // step):
            rows = pl.ds(i * quarter + j * step, step)
            acc[rows] = product(rows, x)
    mark("p04relay")
    landed(left_slot, None, 1)
    push(left_slot, None, 4, mate)
    landed(right_slot, None, 2)
    push(right_slot, None, 5, mate)
    landed(far_slot, None, 3)
    push(far_slot, None, 6, mate)
    mark("p05sidemm")
    landed(xl * 2 + sib, None, 4)
    for i in range(hid.shape[0] // step):
        rows = pl.ds(i * step, step)
        acc[rows] += product(rows, xl)
    mark("p06farwait")
    landed(xr * 2 + sib, None, 5)
    landed(xo * 2 + sib, None, 6)
    mark("p07stats")
    pl.semaphore_wait(wide_sem, 2)
    pl.semaphore_wait(side_sem, 2)
    for d in range(1, ys):
        pl.semaphore_signal(line_sem, inc=1, device_id=at(x, core, y_at[d], z), device_id_type=MESH)
    chosen_load.wait()
    offset = q * weights.shape[2]
    low = q < 2
    order = [jnp.where(low, 3, 0), jnp.where(low, 2, 1)]
    order.append(jnp.where(low, jnp.where(q == 1, 0, 1), jnp.where(q == 2, 3, 2)))
    order.append(q)
    stages = (stage_a, stage_b)

    def rows_of(s, t):
        return pl.ds(pl.multiple_of(order[s] * quarter + t * BLOCK, BLOCK), BLOCK)

    def prepare(s, t):
        rows = rows_of(s, t)
        stages[s % 2][pl.ds(t * BLOCK, BLOCK)] = (acc[rows] + (product(rows, xr) + product(rows, xo))) * LOG2E

    blocks = quarter // BLOCK
    for t in range(blocks):
        prepare(0, t)
    for s in range(4):
        part = order[s]
        for t in range(blocks):
            if s < 3:
                prepare(s + 1, t)
            wanted = chosen_ref[pl.ds(level, 1), rows_of(s, t)] - offset
            for i in range(BLOCK // TILE):
                row = t * (BLOCK // TILE) + i
                scaled = stages[s % 2][pl.ds(row * TILE, TILE)]
                stats = tile_stats(scaled, wanted[:, i * TILE:(i + 1) * TILE])
                for k in range(4):
                    outgoing[part, k, pl.ds(row, 1), :] = stats[k]
        if s < 3:
            copy = pltpu.make_async_remote_copy(
                src_ref=outgoing.at[part], dst_ref=incoming.at[q],
                send_sem=ssend, recv_sem=srecv,
                device_id=at(x, core, y, quad * 4 + part), device_id_type=MESH,
            )
            copy.start()

    mark("p08statwait")
    found = [tuple(outgoing[q, k] for k in range(4))]
    stat_sets = pltpu.make_async_remote_copy(
        src_ref=outgoing.at[pl.ds(0, 3)], dst_ref=incoming.at[pl.ds(0, 3)],
        send_sem=ssend, recv_sem=srecv, device_id=mate, device_id_type=MESH,
    )
    stat_sets.wait_recv()
    for s in range(3):
        found.append(tuple(incoming[order[s], k] for k in range(4)))
    top = functools.reduce(jnp.maximum, [f[0] for f in found])
    total = weighted = picked = jnp.zeros_like(top)
    for own_top, own_total, own_weighted, own_picked in found:
        gap = own_top - top
        factor = jnp.exp2(gap)
        total += factor * own_total
        weighted += factor * (own_weighted + gap * own_total)
        picked += own_picked
    bits = jnp.log(total)
    confidence = (picked - top) * LN2 - bits
    entropy = bits - LN2 * (weighted / total)
    words[cidx] = lax.shift_left(encode(-confidence, CONF_CODE), 16) | encode(entropy, ENT_CODE)

    mark("p09spread")
    pl.semaphore_wait(line_sem, ys - 1)
    for dz in (4, 3, zs - 3, 2, zs - 2, 1, zs - 1, 0):
        for dy in (2, 1, ys - 1, 0):
            if dz or dy:
                pltpu.make_async_remote_copy(
                    src_ref=words.at[cidx], dst_ref=words.at[cidx],
                    send_sem=gsend, recv_sem=grecv,
                    device_id=at(x, core, y_at[dy], z_at[dz]), device_id_type=MESH,
                ).start()
    rest = words.at[pl.ds(0, ys * zs - 1)]
    finals = pltpu.make_async_remote_copy(
        src_ref=rest, dst_ref=rest, send_sem=gsend, recv_sem=grecv, device_id=mate, device_id_type=MESH,
    )
    finals.wait_recv()

    mark("p11drain")
    pltpu.make_async_remote_copy(
        src_ref=weights.at[pl.ds(0, PUSHES)], dst_ref=weights.at[pl.ds(0, PUSHES)],
        send_sem=wsend, recv_sem=wrecv.at[0], device_id=mate, device_id_type=MESH,
    ).wait_send()
    stat_sets.wait_send()
    finals.wait_send()
    mark(None)


def encode(value, code):
    scale, largest = code
    steps = 65535 / math.log1p(largest * scale)
    level = jnp.log(1.0 + jnp.maximum(value, 0.0) * scale) * steps
    return jnp.minimum(level + 0.5, 65535.0).astype(jnp.int32)


def decode(number, code):
    scale, largest = code
    steps = 65535 / math.log1p(largest * scale)
    return (jnp.exp2(number.astype(jnp.float32) * (LOG2E / steps)) - 1.0) * (1 / scale)


def lay_out(words, conf_hbm, ent_hbm, conf, ent, sems):
    levels, rows = conf.shape
    quarter = rows // 4
    copies = []
    for part in range(4):
        found = [words[g * 4 + part] for g in range(levels)]
        fields = (
            (conf, conf_hbm, [-decode(lax.shift_right_logical(w, 16), CONF_CODE) for w in found]),
            (ent, ent_hbm, [decode(w & 65535, ENT_CODE) for w in found]),
        )
        for k, (out, dst, values) in enumerate(fields):
            for j in range(quarter // LANES):
                cols = pl.ds(part * quarter + j * LANES, LANES)
                out[:, cols] = jnp.concatenate([v[j:j + 1] for v in values], axis=0)
            span = pl.ds(part * quarter, quarter)
            copy = pltpu.make_async_copy(out.at[:, span], dst.at[:, span], sems.at[2 * part + k])
            copy.start()
            copies.append(copy)
    for copy in copies:
        copy.wait()


def on_device(xs, ys, zs, hidden, head, chosen):
    rows, width = hidden.shape
    depth, columns = head.shape
    levels = chosen.shape[0]
    quarter = rows // 4
    dma = pltpu.SemaphoreType.DMA
    out = jax.ShapeDtypeStruct((levels, rows), jnp.float32)
    vmem = pl.BlockSpec(memory_space=pltpu.VMEM)
    anywhere = pl.BlockSpec(memory_space=pltpu.HBM)
    words = pl.pallas_call(
        functools.partial(kernel, xs, ys, zs),
        out_shape=pltpu.VMEM((ys * zs, quarter // LANES, LANES), jnp.int32),
        in_specs=[anywhere, anywhere, anywhere],
        out_specs=vmem,
        scratch_shapes=[
            pltpu.VMEM((rows, width), jnp.bfloat16),
            pltpu.VMEM((width // depth, depth, columns), jnp.bfloat16),
            pltpu.VMEM((rows, columns), jnp.float32),
            pltpu.VMEM((quarter, columns), jnp.float32),
            pltpu.VMEM((quarter, columns), jnp.float32),
            pltpu.VMEM((4, 4, quarter // LANES, LANES), jnp.float32),
            pltpu.VMEM((4, 4, quarter // LANES, LANES), jnp.float32),
            pltpu.VMEM((levels, rows), jnp.int32),
            dma((3,)), dma(()), dma((7,)), dma(()), dma(()), dma(()), dma(()),
            pltpu.SemaphoreType.REGULAR, pltpu.SemaphoreType.REGULAR,
            pltpu.SemaphoreType.REGULAR, pltpu.SemaphoreType.REGULAR,
        ],
        compiler_params=pltpu.CompilerParams(collective_id=0, has_side_effects=True, vmem_limit_bytes=56 << 20),
    )(hidden, head, chosen)
    return pl.pallas_call(
        lay_out,
        out_shape=(out, out),
        in_specs=[vmem],
        out_specs=(anywhere, anywhere),
        scratch_shapes=[pltpu.VMEM((levels, rows), jnp.float32)] * 2 + [dma((8,))],
        compiler_params=pltpu.CompilerParams(vmem_limit_bytes=4 << 20),
    )(words)


def solution(mesh):
    return jax.shard_map(
        functools.partial(on_device, mesh.shape["frames"] // 2, 4, mesh.shape["codes"] // 4),
        mesh=mesh,
        in_specs=(P("frames", None), P("frames", "codes"), P(None, "frames")),
        out_specs=(P(None, "frames"), P(None, "frames")),
        check_vma=False,
    )
```
